512 devices in a mesh: ctx: 64 (over x, z), head: 8 (over y, core).
Axes of the slice: x: 4, y: 4, z: 16, core: 2. Of those that a mesh axis runs over, the one named last changes fastest.
Arguments:
- queries: bfloat16 [32768, 4096], P('ctx', 'head'), may hold values from -6 to 6
- key_rows: bfloat16 [32768, 4096], P('ctx', 'head'), may hold values from -6 to 6
- value_rows: bfloat16 [32768, 4096], P('ctx', 'head'), may hold values from -6 to 6
- decay_rates: float32 [32], P('head'), as said below
- norm_gain: float32 [4096], P('head'), may hold values from 0.5 to 1.5
- out_grad: bfloat16 [32768, 4096], P('ctx', 'head'), may hold values from -6 to 6
Outputs:
- normed_out: bfloat16 [32768, 4096], P('ctx', 'head')
- query_grad: bfloat16 [32768, 4096], P('ctx', 'head')
- key_grad: bfloat16 [32768, 4096], P('ctx', 'head')
- value_grad: bfloat16 [32768, 4096], P('ctx', 'head')
The draws below stay inside these ranges and needn't reach their ends.
Inputs may be any that keep to these rules, and one draw needn't show every extreme that they name: `decay_rates`: each head's decay factor per token is exp(-rate).
All inputs are finite; a program needn't handle non-finite values.
Results may differ from the reference program's by a relative error of at most 0.005.
Values sent between devices are 32-bit elements; how exact they have to be, the bound alone decides.
No kernel may reach another device: no remote copies, remote signals or barrier semaphores. Data moves between devices by JAX's collectives and lax.ppermute only.
A program may use at most 64 MiB of HBM per device.

```python
import jax
import jax.numpy as jnp
from jax import lax

DK = 128
BLOCK = 256
HEADS = 32
TOKENS = 32768


def draw_decay_rates(key, part):
    picker, slow_key, fast_key = jax.random.split(key, 3)
    share = 0.5
    slow_rates = jnp.exp(jax.random.uniform(slow_key, (HEADS,), jnp.float32, jnp.log(0.5 / TOKENS), jnp.log(2.0 / TOKENS)))
    fast_rates = jnp.exp(jax.random.uniform(fast_key, (HEADS,), jnp.float32, jnp.log(0.02), jnp.log(0.05)))
    chosen = jax.random.uniform(picker, (HEADS,), jnp.float32) < share
    return jnp.where(chosen, slow_rates, fast_rates)


def levels(key, dims, cuts, least, top_value):
    factor_of, own = 1.0, jax.random.fold_in(key, 6)
    for dim, shards_of in cuts:
        steps = jnp.exp(jax.random.uniform(jax.random.fold_in(own, dim), (shards_of,), jnp.float32, least / len(cuts), top_value / len(cuts)))
        factor_of = factor_of * jnp.repeat(steps, dims[dim] // shards_of).reshape([-1 if axis == dim else 1 for axis in range(len(dims))])
    return factor_of


def bell_draw(rng, dims, spread, most, pieces=(), kind=jnp.bfloat16):
    level = levels(rng, dims, pieces, -0.22, 0.18) if pieces else 1.0
    entries = jax.random.normal(rng, dims, jnp.float32) * spread * level
    return jnp.minimum(jnp.maximum(entries, -most), most).astype(kind)


def setup_inputs(seed: int = 0) -> dict:
    splits = jax.random.split(jax.random.key(seed), 7)
    return {
        "queries": bell_draw(splits[0], (TOKENS, HEADS * DK), 1.0, 6.0, ((0, 64), (1, 8))),
        "key_rows": bell_draw(splits[1], (TOKENS, HEADS * DK), 1.0, 6.0, ((0, 64), (1, 8))),
        "value_rows": bell_draw(splits[2], (TOKENS, HEADS * DK), 1.0, 6.0, ((0, 64), (1, 8))),
        "decay_rates": draw_decay_rates(jax.random.fold_in(splits[6], 71), 0),
        "norm_gain": jnp.clip(1.0 + 0.1 * jax.random.normal(splits[4], (HEADS * DK,), jnp.float32), 0.5, 1.5),
        "out_grad": bell_draw(splits[5], (TOKENS, HEADS * DK), 1.0, 6.0, ((0, 64), (1, 8))),
    }


highest = lax.Precision.HIGHEST
epsilon = 1e-06

def exact_product(form, left, right):
    return jnp.einsum(form, left.astype(jnp.float32), right.astype(jnp.float32), precision=highest)

def decay_tables(decay_rates, length):
    position = jnp.arange(length, dtype=jnp.float32)
    spacing = position[:, None] - position[None, :]
    weights = jnp.where(spacing[None] >= 0, jnp.exp(-decay_rates[:, None, None] * jnp.maximum(spacing, 0.0)[None]), 0.0)
    leading = jnp.exp(-decay_rates[None, :] * (position[:, None] + 1.0))
    trailing = jnp.exp(-decay_rates[None, :] * (length - 1.0 - position[:, None]))
    after_end = jnp.exp(-decay_rates[None, :] * (length - position[:, None]))
    from_start = jnp.exp(-decay_rates[None, :] * position[:, None])
    return (weights, leading, trailing, after_end, from_start)

def reference(queries, key_rows, value_rows, decay_rates, norm_gain, out_grad):
    token_count = queries.shape[0]
    head_count = decay_rates.shape[0]
    head_width = queries.shape[1] // head_count
    block_count = token_count // BLOCK
    weights, leading, trailing, after_end, from_start = decay_tables(decay_rates, BLOCK)
    full_decay = jnp.exp(-decay_rates * BLOCK)[:, None, None]

    def blocked(array):
        return array.reshape(block_count, BLOCK, head_count, head_width)
    query_blocks = blocked(queries)
    key_blocks = blocked(key_rows)
    value_blocks = blocked(value_rows)
    initial = jnp.zeros((head_count, head_width, head_width), jnp.float32)

    def advance(memory, blocks):
        query_rows, key_part, value_part = blocks
        scores = exact_product('ihd,jhd->hij', query_rows, key_part)
        attn_probs = (scores * weights).astype(jnp.bfloat16)
        inside = exact_product('hij,jhd->ihd', attn_probs, value_part)
        carried = exact_product('iha,hac->ihc', query_rows, memory) * leading[:, :, None]
        update = exact_product('jha,jhc->hac', key_part.astype(jnp.float32) * trailing[:, :, None], value_part)
        return (full_decay * memory + update, inside + carried)
    _, outputs = lax.scan(advance, initial, (query_blocks, key_blocks, value_blocks))
    flat = outputs.reshape(token_count, head_count * head_width)
    features = float(head_count * head_width)
    scale = lax.rsqrt(lax.optimization_barrier(jnp.sum(flat * flat, axis=1)) / features + epsilon)
    normed = flat * scale[:, None]
    normed_out = (normed * norm_gain[None, :]).astype(jnp.bfloat16)
    grad_normed = out_grad.astype(jnp.float32) * norm_gain[None, :]
    coeff = scale * lax.optimization_barrier(jnp.sum(grad_normed * flat, axis=1)) / features
    grad_attn = (scale[:, None] * (grad_normed - normed * coeff[:, None])).astype(jnp.bfloat16)
    grad_blocks = blocked(grad_attn)

    def forward_grad(memory, blocks):
        query_rows, key_part, value_part, grad_rows = blocks
        grad_scores = exact_product('ihc,jhc->hij', grad_rows, value_part)
        grad_probs = (grad_scores * weights).astype(jnp.bfloat16)
        query_part = exact_product('hij,jha->iha', grad_probs, key_part)
        query_part = query_part + exact_product('ihc,hac->iha', grad_rows, memory) * leading[:, :, None]
        update = exact_product('jha,jhc->hac', key_part.astype(jnp.float32) * trailing[:, :, None], value_part)
        return (full_decay * memory + update, query_part)
    _, query_grad = lax.scan(forward_grad, initial, (query_blocks, key_blocks, value_blocks, grad_blocks))

    def backward_grad(backlog, blocks):
        query_rows, key_part, value_part, grad_rows = blocks
        scores = exact_product('ihd,jhd->hij', query_rows, key_part)
        attn_probs = (scores * weights).astype(jnp.bfloat16)
        grad_scores = exact_product('ihc,jhc->hij', grad_rows, value_part)
        grad_probs = (grad_scores * weights).astype(jnp.bfloat16)
        key_out = exact_product('hij,iha->jha', grad_probs, query_rows)
        key_out = key_out + exact_product('jhc,hac->jha', value_part, backlog) * after_end[:, :, None]
        value_out = exact_product('hij,ihc->jhc', attn_probs, grad_rows)
        value_out = value_out + exact_product('jha,hac->jhc', key_part, backlog) * after_end[:, :, None]
        gathered = exact_product('iha,ihc->hac', query_rows.astype(jnp.float32) * from_start[:, :, None], grad_rows)
        return (full_decay * backlog + gathered, (key_out, value_out))
    _, (key_grad, value_grad) = lax.scan(backward_grad, initial, (query_blocks, key_blocks, value_blocks, grad_blocks), reverse=True)

    def flatten(array):
        return array.reshape(token_count, head_count * head_width).astype(jnp.bfloat16)
    return (normed_out, flatten(query_grad), flatten(key_grad), flatten(value_grad))
```

```python
import functools

import jax
import jax.numpy as jnp
from jax import lax
from jax.experimental import pallas as pl
from jax.experimental.pallas import tpu as pltpu
from jax.sharding import Mesh
from jax.sharding import PartitionSpec as P

BLOCK = 256
LINE = ("ctx_0", "ctx_1")
EPSILON = 1e-06
F32 = jnp.float32
BF16 = jnp.bfloat16
SMEM = pl.BlockSpec(memory_space=pltpu.SMEM)
VMEM = pl.BlockSpec(memory_space=pltpu.VMEM)


def dot(left, right, left_dim, right_dim):
    return lax.dot_general(
        left, right, (((left_dim,), (right_dim,)), ((), ())), preferred_element_type=F32
    )


def halves(wide):
    high = wide.astype(BF16)
    return high, (wide - high.astype(F32)).astype(BF16)


def dot_wide_right(left, right, left_dim, right_dim):
    high, low = halves(right)
    return dot(left, high, left_dim, right_dim) + dot(left, low, left_dim, right_dim)


def dot_wide_left(left, right, left_dim, right_dim):
    high, low = halves(left)
    return dot(high, right, left_dim, right_dim) + dot(low, right, left_dim, right_dim)


def rows_of(shape):
    return lax.broadcasted_iota(jnp.int32, shape, 0).astype(F32)


def decay_weights(rate):
    shape = (BLOCK, BLOCK)
    spacing = rows_of(shape) - lax.broadcasted_iota(jnp.int32, shape, 1).astype(F32)
    return jnp.where(spacing >= 0, jnp.exp(-rate * jnp.maximum(spacing, 0.0)), 0.0)


def block_rows(block):
    return slice(block * BLOCK, (block + 1) * BLOCK)


def memory_kernel(rates, keys, values, end, first):
    rate = rates[pl.program_id(0)]
    trailing = jnp.exp(-rate * (BLOCK - 1.0 - rows_of((BLOCK, 128))))
    full = jnp.exp(jnp.full((128, 128), -BLOCK * rate, F32))
    memory = None
    for block in range(2):
        rows = block_rows(block)
        update = dot_wide_left(keys[rows, :].astype(F32) * trailing, values[rows, :], 0, 0)
        memory = update if memory is None else full * memory + update
        if block == 0:
            first[0] = memory
    end[0] = memory


def inside_kernel(rates, queries, keys, values, probs, inside):
    weights = decay_weights(rates[pl.program_id(0)])
    for block in range(2):
        rows = block_rows(block)
        scores = dot(queries[rows, :], keys[rows, :], 1, 1)
        low = (scores * weights).astype(BF16)
        probs[0, block] = low
        inside[rows, :] = dot(low, values[rows, :], 1, 0)


def carried_kernel(
    rates, queries, entering, first, inside, gain, out_grad, attention, sums, squares, projection
):
    head = pl.program_id(0)
    rate = rates[head]
    leading = jnp.exp(-rate * (rows_of((BLOCK, 128)) + 1.0))
    full = jnp.exp(jnp.full((128, 128), -BLOCK * rate, F32))
    memory = entering[0]
    for block in range(2):
        rows = block_rows(block)
        carried = dot_wide_right(queries[rows, :], memory, 1, 0) * leading
        out = inside[rows, :] + carried
        attention[rows, :] = out
        grad = out_grad[rows, :].astype(F32) * gain[...]
        square, product = out * out, grad * out

        @pl.when(head == 0)
        def _():
            squares[rows, :] = square
            projection[rows, :] = product

        @pl.when(head > 0)
        def _():
            squares[rows, :] += square
            projection[rows, :] += product

        memory = full * memory + first[0]

    @pl.when(head == pl.num_programs(0) - 1)
    def _():
        flat = []
        for part in (squares, projection):
            for tile in range(4):
                turned = part[tile * 128 : (tile + 1) * 128, :].T
                flat.append(jnp.sum(turned, axis=0, keepdims=True))
        sums[...] = jnp.concatenate(flat, axis=0)


def grad_kernel(
    features, rates, sums, queries, attention, gain, out_grad, grad_out, normed_out, end, second, scale, coeff
):
    head = pl.program_id(0)
    rate = rates[head]
    @pl.when(head == 0)
    def _():
        scale_row = lax.rsqrt(sums[0:4] / features + EPSILON)
        coeff_row = scale_row * sums[4:8] / features
        for tile in range(4):
            rows = slice(tile * 128, (tile + 1) * 128)
            scale[rows, :] = jnp.broadcast_to(scale_row[tile : tile + 1], (128, 128)).T
            coeff[rows, :] = jnp.broadcast_to(coeff_row[tile : tile + 1], (128, 128)).T

    start = jnp.exp(-rate * rows_of((BLOCK, 128)))
    full = jnp.exp(jnp.full((128, 128), -BLOCK * rate, F32))
    backlog = None
    for block in (1, 0):
        rows = block_rows(block)
        by = scale[rows, :]
        normed = attention[rows, :] * by
        normed_out[rows, :] = (normed * gain[...]).astype(BF16)
        grad = out_grad[rows, :].astype(F32) * gain[...]
        low = (by * (grad - normed * coeff[rows, :])).astype(BF16)
        grad_out[rows, :] = low
        gathered = dot_wide_left(queries[rows, :].astype(F32) * start, low, 0, 0)
        backlog = gathered if backlog is None else full * backlog + gathered
        if block == 1:
            second[0] = backlog
    end[0] = backlog


def local_kernel(
    rates, queries, keys, values, grads, probs, entering, first, query_grad, key_part, value_part
):
    rate = rates[pl.program_id(0)]
    weights = decay_weights(rate)
    leading = jnp.exp(-rate * (rows_of((BLOCK, 128)) + 1.0))
    full = jnp.exp(jnp.full((128, 128), -BLOCK * rate, F32))
    memory = entering[0]
    for block in range(2):
        rows = block_rows(block)
        grad = grads[rows, :]
        low = (dot(grad, values[rows, :], 1, 1) * weights).astype(BF16)
        carried = dot_wide_right(grad, memory, 1, 1) * leading
        query_grad[rows, :] = (dot(low, keys[rows, :], 1, 0) + carried).astype(BF16)
        key_part[rows, :] = dot(low, queries[rows, :], 0, 0)
        value_part[rows, :] = dot(probs[0, block], grad, 0, 0)
        memory = full * memory + first[0]


def finish_kernel(rates, keys, values, key_part, value_part, after, second, key_grad, value_grad):
    rate = rates[pl.program_id(0)]
    ending = jnp.exp(-rate * (BLOCK - rows_of((BLOCK, 128))))
    full = jnp.exp(jnp.full((128, 128), -BLOCK * rate, F32))
    backlog = after[0]
    for block in (1, 0):
        rows = block_rows(block)
        key_more = dot_wide_right(values[rows, :], backlog, 1, 1) * ending
        value_more = dot_wide_right(keys[rows, :], backlog, 1, 0) * ending
        key_grad[rows, :] = (key_part[rows, :] + key_more).astype(BF16)
        value_grad[rows, :] = (value_part[rows, :] + value_more).astype(BF16)
        backlog = full * backlog + second[0]


def shape(*dims, dtype=F32):
    return jax.ShapeDtypeStruct(dims, dtype)


COLS = pl.BlockSpec((512, 128), lambda h: (0, h))
GAIN = pl.BlockSpec((1, 128), lambda h: (0, h))
STATE = pl.BlockSpec((1, 128, 128), lambda h: (h, 0, 0))
PROBS = pl.BlockSpec((1, 2, BLOCK, BLOCK), lambda h: (h, 0, 0, 0))


def whole(*dims):
    return pl.BlockSpec(dims, lambda h: (0,) * len(dims))


def per_head(kernel, name, in_specs, outs, out_specs, scratch=(), flops=50_000_000):
    return pl.pallas_call(
        kernel,
        grid=(4,),
        in_specs=[SMEM] + in_specs,
        out_specs=out_specs,
        out_shape=outs,
        scratch_shapes=scratch,
        name=name,
        cost_estimate=pl.CostEstimate(flops=flops, bytes_accessed=4_000_000, transcendentals=300_000),
        compiler_params=pltpu.CompilerParams(dimension_semantics=("arbitrary",)),
    )


def scan_total(table, pieces, reverse):
    count, rows, lanes = pieces.shape

    def kernel(table_ref, piece_ref, total_ref):
        order = range(count - 1, -1, -1) if reverse else range(count)
        running = None
        for k in order:
            piece = piece_ref[k]
            running = piece if running is None else running * table_ref[0] + piece
        for peer in range(total_ref.shape[0]):
            total_ref[peer] = running

    return pl.pallas_call(
        kernel,
        in_specs=[SMEM, VMEM],
        out_specs=VMEM,
        out_shape=shape(lax.axis_size(LINE[0]), rows, lanes),
        name="scan_total",
    )(table, pieces)


def scan_prefix(table, pieces, totals, reverse):
    count, rows, lanes = pieces.shape
    first = 5 if reverse else 1

    def kernel(table_ref, piece_ref, total_ref, prefix_ref):
        order = list(range(count - 1, -1, -1) if reverse else range(count))
        running = total_ref[0] * table_ref[first]
        for peer in range(1, total_ref.shape[0]):
            running = running + total_ref[peer] * table_ref[first + peer]
        for k in order:
            prefix_ref[k] = running
            if k != order[-1]:
                running = running * table_ref[0] + piece_ref[k]

    return pl.pallas_call(
        kernel,
        in_specs=[SMEM, VMEM, VMEM],
        out_specs=VMEM,
        out_shape=shape(count, rows, lanes),
        name="scan_prefix",
    )(table, pieces, totals)


def line_table(decay_rates, token_count):
    far, near = lax.axis_index(LINE[0]), lax.axis_index(LINE[1])
    far_size, near_size = lax.axis_size(LINE[0]), lax.axis_size(LINE[1])
    rate = lax.dynamic_index_in_dim(
        decay_rates, near * decay_rates.shape[0] // near_size, 0, keepdims=False
    )
    slot = jnp.arange(1 + 2 * far_size)
    earlier = far - slot
    later = slot - 1 - far_size - far - 1
    steps = jnp.where(slot > far_size, later, earlier) * near_size
    steps = jnp.where(slot == 0, 1, steps)
    weights = jnp.exp(-rate * token_count * jnp.maximum(steps, 0).astype(F32))
    return jnp.where(steps >= 0, weights, 0.0)


def along_context(table, state, reverse):
    near_size, far_size = lax.axis_size(LINE[1]), lax.axis_size(LINE[0])
    lanes = state.shape[-1]
    pieces = lax.all_to_all(state.reshape(near_size, -1, lanes), LINE[1], 0, 0)
    totals = lax.all_to_all(scan_total(table, pieces, reverse), LINE[0], 0, 0)
    prefix = scan_prefix(table, pieces, totals, reverse)
    return lax.all_to_all(prefix, LINE[1], 0, 0).reshape(state.shape)


def on_device(queries, key_rows, value_rows, decay_rates, norm_gain, out_grad):
    tokens, width = queries.shape
    heads = decay_rates.shape[0]
    features = float(width * lax.axis_size("head"))
    gain = norm_gain[None, :]
    table = line_table(decay_rates, tokens)
    state = shape(heads, 128, 128)
    wide, narrow = shape(tokens, width), shape(tokens, width, dtype=BF16)
    memory_end, memory_first = per_head(
        memory_kernel, "memory", [COLS, COLS], (state, state), (STATE, STATE)
    )(decay_rates, key_rows, value_rows)
    probs, inside = per_head(
        inside_kernel,
        "inside",
        [COLS, COLS, COLS],
        (shape(heads, 2, BLOCK, BLOCK, dtype=BF16), wide),
        (PROBS, COLS),
    )(decay_rates, queries, key_rows, value_rows)
    entering = along_context(table, memory_end, False)
    attention, sums = per_head(
        carried_kernel,
        "carried",
        [COLS, STATE, STATE, COLS, GAIN, COLS],
        (wide, shape(8, 128)),
        (COLS, whole(8, 128)),
        [pltpu.VMEM((tokens, 128), F32), pltpu.VMEM((tokens, 128), F32)],
    )(decay_rates, queries, entering, memory_first, inside, gain, out_grad)
    sums = lax.psum(sums, "head")
    grads, normed_out, backlog_end, backlog_second = per_head(
        functools.partial(grad_kernel, features),
        "grad",
        [whole(8, 128), COLS, COLS, GAIN, COLS],
        (narrow, narrow, state, state),
        (COLS, COLS, STATE, STATE),
        [pltpu.VMEM((tokens, 128), F32), pltpu.VMEM((tokens, 128), F32)],
    )(decay_rates, sums, queries, attention, gain, out_grad)
    query_grad, key_part, value_part = per_head(
        local_kernel,
        "local",
        [COLS, COLS, COLS, COLS, PROBS, STATE, STATE],
        (narrow, wide, wide),
        (COLS, COLS, COLS),
    )(decay_rates, queries, key_rows, value_rows, grads, probs, entering, memory_first)
    after = along_context(table, backlog_end, True)
    key_grad, value_grad = per_head(
        finish_kernel,
        "finish",
        [COLS, COLS, COLS, COLS, STATE, STATE],
        (narrow, narrow),
        (COLS, COLS),
    )(decay_rates, key_rows, value_rows, key_part, value_part, after, backlog_second)
    return (normed_out, query_grad, key_grad, value_grad)


def solution(mesh):
    split = Mesh(mesh.devices.reshape(4, 16, mesh.shape["head"]), LINE + ("head",))
    rows = P(LINE, "head")
    return jax.shard_map(
        on_device,
        mesh=split,
        in_specs=(rows, rows, rows, P("head"), P("head"), rows),
        out_specs=(rows, rows, rows, rows),
        check_vma=False,
    )
```

```python
import dataclasses
import functools

import jax
import jax.numpy as jnp
from jax import lax
from jax.experimental import pallas as pl
from jax.experimental.pallas import tpu as pltpu
from jax.sharding import Mesh
from jax.sharding import PartitionSpec as P

BLOCK = 256
LINE = ("ctx_0", "ctx_1")
SIDE = ("row", "core")
EPSILON = 1e-06
GRANT = 12 << 20
F32 = jnp.float32
BF16 = jnp.bfloat16
SMEM = pl.BlockSpec(memory_space=pltpu.SMEM)
VMEM = pl.BlockSpec(memory_space=pltpu.VMEM)


def dot(left, right, left_dim, right_dim):
    return lax.dot_general(
        left, right, (((left_dim,), (right_dim,)), ((), ())), preferred_element_type=F32
    )


def halves(wide):
    high = wide.astype(BF16)
    return high, (wide - high.astype(F32)).astype(BF16)


def dot_wide_right(left, right, left_dim, right_dim):
    high, low = halves(right)
    return dot(left, high, left_dim, right_dim) + dot(left, low, left_dim, right_dim)


def dot_wide_left(left, right, left_dim, right_dim):
    high, low = halves(left)
    return dot(high, right, left_dim, right_dim) + dot(low, right, left_dim, right_dim)


def rows_of(shape):
    return lax.broadcasted_iota(jnp.int32, shape, 0).astype(F32)


def decay_weights(rate):
    shape = (BLOCK, BLOCK)
    spacing = rows_of(shape) - lax.broadcasted_iota(jnp.int32, shape, 1).astype(F32)
    return jnp.where(spacing >= 0, jnp.exp(-rate * jnp.maximum(spacing, 0.0)), 0.0)


def block_rows(block):
    return slice(block * BLOCK, (block + 1) * BLOCK)


@dataclasses.dataclass
class Streamed:
    array: object


def cols_of(head):
    return slice(head * 128, (head + 1) * 128)


def memory_kernel(rates, keys, values, end, first):
    rows_in = rows_of((BLOCK, 128))
    for head in range(4):
        cols = cols_of(head)
        trailing = jnp.exp(-rates[head] * (BLOCK - 1.0 - rows_in))
        full = jnp.exp(jnp.full((128, 128), -BLOCK * rates[head], F32))
        updates = []
        for block in range(2):
            rows = block_rows(block)
            wide = keys[rows, cols].astype(F32) * trailing
            updates.append(dot_wide_left(wide, values[rows, cols], 0, 0))
        first[head] = updates[0]
        end[head] = full * updates[0] + updates[1]


def inside_kernel(rates, queries, keys, values, probs, inside):
    for head in range(4):
        cols = cols_of(head)
        weights = decay_weights(rates[head])
        for block in range(2):
            rows = block_rows(block)
            scores = dot(queries[rows, cols], keys[rows, cols], 1, 1)
            low = (scores * weights).astype(BF16)
            probs[head, block] = low
            inside[rows, cols] = dot(low, values[rows, cols], 1, 0)


def carried_kernel(rates, queries, entering, first, inside, gain, out_grad, attention, sums):
    after_start = rows_of((BLOCK, 128)) + 1.0
    squares, products = [], []
    for block in range(2):
        rows = block_rows(block)
        square = product = None
        for head in range(4):
            cols = cols_of(head)
            memory = entering[head]
            if block == 1:
                full = jnp.exp(jnp.full((128, 128), -BLOCK * rates[head], F32))
                memory = full * memory + first[head]
            leading = jnp.exp(-rates[head] * after_start)
            carried = dot_wide_right(queries[rows, cols], memory, 1, 0) * leading
            out = inside[rows, cols] + carried
            attention[rows, cols] = out
            grad = out_grad[rows, cols].astype(F32) * gain[:, cols]
            square = out * out if square is None else square + out * out
            product = grad * out if product is None else product + grad * out
        for part, flat in ((square, squares), (product, products)):
            for tile in range(2):
                turned = part[tile * 128 : (tile + 1) * 128, :].T
                flat.append(jnp.sum(turned, axis=0, keepdims=True))
    sums[...] = jnp.concatenate(squares + products, axis=0)


def per_token(row):
    return jnp.broadcast_to(row, (128, 128)).T


def scales_of(features, sums, block):
    scale = lax.rsqrt(sums[0:4] / features + EPSILON)
    coeff = scale * sums[4:8] / features
    tiles = (2 * block, 2 * block + 1)
    return tuple(
        jnp.concatenate([per_token(part[tile : tile + 1]) for tile in tiles], axis=0)
        for part in (scale, coeff)
    )


def attention_grad(attention, out_grad, gain, scale, coeff):
    normed = attention * scale
    grad = out_grad.astype(F32) * gain
    return normed, (scale * (grad - normed * coeff)).astype(BF16)


def grad_kernel(features, rates, sums, queries, attention, gain, out_grad, end, second):
    from_start = rows_of((BLOCK, 128))
    for block in (1, 0):
        rows = block_rows(block)
        scale, coeff = scales_of(features, sums, block)
        for head in range(4):
            cols = cols_of(head)
            _, low = attention_grad(
                attention[rows, cols], out_grad[rows, cols], gain[:, cols], scale, coeff
            )
            start = jnp.exp(-rates[head] * from_start)
            gathered = dot_wide_left(queries[rows, cols].astype(F32) * start, low, 0, 0)
            if block == 1:
                second[head] = gathered
            else:
                full = jnp.exp(jnp.full((128, 128), -BLOCK * rates[head], F32))
                end[head] = full * second[head] + gathered


def local_kernel(
    features,
    rates,
    queries,
    keys,
    values,
    out_grad,
    probs,
    entering,
    first,
    sums,
    attention,
    gain,
    query_grad,
    normed_out,
    key_part,
    value_part,
):
    after_start = rows_of((BLOCK, 128)) + 1.0
    for block in range(2):
        rows = block_rows(block)
        scale, coeff = scales_of(features, sums, block)
        for head in range(4):
            cols = cols_of(head)
            weights = decay_weights(rates[head])
            memory = entering[head]
            if block == 1:
                full = jnp.exp(jnp.full((128, 128), -BLOCK * rates[head], F32))
                memory = full * memory + first[head]
            leading = jnp.exp(-rates[head] * after_start)
            normed, grad = attention_grad(
                attention[rows, cols], out_grad[rows, cols], gain[:, cols], scale, coeff
            )
            normed_out[rows, cols] = (normed * gain[:, cols]).astype(BF16)
            low = (dot(grad, values[rows, cols], 1, 1) * weights).astype(BF16)
            carried = dot_wide_right(grad, memory, 1, 1) * leading
            query_grad[rows, cols] = (dot(low, keys[rows, cols], 1, 0) + carried).astype(BF16)
            key_part[rows, cols] = dot(low, queries[rows, cols], 0, 0)
            value_part[rows, cols] = dot(probs[head, block], grad, 0, 0)


def finish_kernel(
    rates, keys, values, key_part, value_part, after, second, key_grad, value_grad
):
    tile = pl.program_id(0)
    to_end = BLOCK - rows_of((128, 128)) - 128.0 * (tile % 2).astype(F32)
    for head in range(4):
        cols = cols_of(head)
        ending = jnp.exp(-rates[head] * to_end)
        full = jnp.exp(jnp.full((128, 128), -BLOCK * rates[head], F32))
        backlog = jnp.where(tile < 2, full * after[head] + second[head], after[head])
        key_more = dot_wide_right(values[:, cols], backlog, 1, 1) * ending
        value_more = dot_wide_right(keys[:, cols], backlog, 1, 0) * ending
        key_grad[:, cols] = (key_part[:, cols] + key_more).astype(BF16)
        value_grad[:, cols] = (value_part[:, cols] + value_more).astype(BF16)


def shape(*dims, dtype=F32):
    return jax.ShapeDtypeStruct(dims, dtype)


def near(array):
    return pltpu.with_memory_space_constraint(array, pltpu.VMEM)


def call(kernel, name, outs, *operands, grant=GRANT):
    rates, *rest = operands
    streamed = [isinstance(array, Streamed) for array in rest]
    arrays = [array.array if isinstance(array, Streamed) else array for array in rest]
    far = pl.BlockSpec()
    return pl.pallas_call(
        kernel,
        in_specs=[SMEM] + [far if flag else VMEM for flag in streamed],
        out_specs=tuple(far if isinstance(out, Streamed) else VMEM for out in outs),
        out_shape=tuple(out.array if isinstance(out, Streamed) else out for out in outs),
        name=name,
        cost_estimate=pl.CostEstimate(
            flops=400_000_000, bytes_accessed=4_000_000, transcendentals=300_000
        ),
        compiler_params=pltpu.CompilerParams(vmem_limit_bytes=grant),
    )(rates, *arrays)


def scan_total(table, pieces, reverse):
    count, rows, lanes = pieces.shape

    def kernel(table_ref, piece_ref, total_ref):
        order = range(count - 1, -1, -1) if reverse else range(count)
        running = None
        for k in order:
            piece = piece_ref[k]
            running = piece if running is None else running * table_ref[0] + piece
        for peer in range(total_ref.shape[0]):
            total_ref[peer] = running

    return pl.pallas_call(
        kernel,
        in_specs=[SMEM, VMEM],
        out_specs=VMEM,
        out_shape=pltpu.VMEM((lax.axis_size(LINE[0]), rows, lanes), F32),
        name="scan_total",
        compiler_params=pltpu.CompilerParams(vmem_limit_bytes=GRANT),
    )(table, near(pieces))


def scan_prefix(table, pieces, totals, reverse):
    count, rows, lanes = pieces.shape
    first = 5 if reverse else 1

    def kernel(table_ref, piece_ref, total_ref, prefix_ref):
        order = list(range(count - 1, -1, -1) if reverse else range(count))
        running = total_ref[0] * table_ref[first]
        for peer in range(1, total_ref.shape[0]):
            running = running + total_ref[peer] * table_ref[first + peer]
        for k in order:
            prefix_ref[k] = running
            if k != order[-1]:
                running = running * table_ref[0] + piece_ref[k]

    return pl.pallas_call(
        kernel,
        in_specs=[SMEM, VMEM, VMEM],
        out_specs=VMEM,
        out_shape=pltpu.VMEM((count, rows, lanes), F32),
        name="scan_prefix",
        compiler_params=pltpu.CompilerParams(vmem_limit_bytes=GRANT),
    )(table, near(pieces), near(totals))


def line_table(decay_rates, token_count):
    far, near = lax.axis_index(LINE[0]), lax.axis_index(LINE[1])
    far_size, near_size = lax.axis_size(LINE[0]), lax.axis_size(LINE[1])
    rate = lax.dynamic_index_in_dim(
        decay_rates, near * decay_rates.shape[0] // near_size, 0, keepdims=False
    )
    slot = jnp.arange(1 + 2 * far_size)
    earlier = far - slot
    later = slot - 1 - far_size - far - 1
    steps = jnp.where(slot > far_size, later, earlier) * near_size
    steps = jnp.where(slot == 0, 1, steps)
    weights = jnp.exp(-rate * token_count * jnp.maximum(steps, 0).astype(F32))
    return jnp.where(steps >= 0, weights, 0.0)


def along_context(table, state, reverse):
    near_size, far_size = lax.axis_size(LINE[1]), lax.axis_size(LINE[0])
    lanes = state.shape[-1]
    pieces = lax.all_to_all(state.reshape(near_size, -1, lanes), LINE[1], 0, 0)
    totals = lax.all_to_all(scan_total(table, pieces, reverse), LINE[0], 0, 0)
    prefix = scan_prefix(table, pieces, totals, reverse)
    return lax.all_to_all(prefix, LINE[1], 0, 0).reshape(state.shape)


def on_device(queries, key_rows, value_rows, decay_rates, norm_gain, out_grad):
    tokens, width = queries.shape
    heads = decay_rates.shape[0]
    features = float(width * lax.axis_size(SIDE))
    gain = norm_gain[None, :]
    table = line_table(decay_rates, tokens)
    state = shape(heads, 128, 128)
    wide, narrow = shape(tokens, width), shape(tokens, width, dtype=BF16)
    tables = shape(heads, 2, BLOCK, BLOCK, dtype=BF16)
    state_near, wide_near = pltpu.VMEM(state.shape, F32), pltpu.VMEM(wide.shape, F32)
    far_q, far_k, far_v, far_grad = map(Streamed, (queries, key_rows, value_rows, out_grad))
    memory_end, memory_first = call(
        memory_kernel,
        "memory",
        (state_near, state_near),
        decay_rates,
        near(key_rows),
        near(value_rows),
    )
    probs, inside = call(
        inside_kernel,
        "inside",
        (Streamed(tables), wide_near),
        decay_rates,
        far_q,
        far_k,
        far_v,
        grant=None,
    )
    entering = along_context(table, memory_end, False)
    attention, sums = call(
        carried_kernel,
        "carried",
        (wide_near, pltpu.VMEM((8, 128), F32)),
        decay_rates,
        near(queries),
        near(entering),
        near(memory_first),
        near(inside),
        near(gain),
        near(out_grad),
    )
    sums = lax.psum(lax.psum(sums, "core"), "row")
    backlog_end, backlog_second = call(
        functools.partial(grad_kernel, features),
        "grad",
        (state_near, state_near),
        decay_rates,
        near(sums),
        near(queries),
        near(attention),
        near(gain),
        near(out_grad),
    )
    query_grad, normed_out, key_part, value_part = call(
        functools.partial(local_kernel, features),
        "local",
        (Streamed(narrow), Streamed(narrow), Streamed(wide), Streamed(wide)),
        decay_rates,
        far_q,
        far_k,
        far_v,
        far_grad,
        Streamed(probs),
        near(entering),
        near(memory_first),
        near(sums),
        near(attention),
        near(gain),
        grant=None,
    )
    after = along_context(table, backlog_end, True)
    tile_rows = pl.BlockSpec((128, width), lambda tile: (tile, 0))
    key_grad, value_grad = pl.pallas_call(
        finish_kernel,
        grid=(tokens // 128,),
        in_specs=[SMEM] + [tile_rows] * 4 + [VMEM] * 2,
        out_specs=(tile_rows, tile_rows),
        out_shape=(narrow, narrow),
        name="finish",
    )(
        decay_rates,
        key_rows,
        value_rows,
        key_part,
        value_part,
        near(after),
        near(backlog_second),
    )
    return (normed_out, query_grad, key_grad, value_grad)


def solution(mesh):
    split = Mesh(mesh.devices.reshape(4, 16, 4, 2), LINE + SIDE)
    rows = P(LINE, SIDE)
    return jax.shard_map(
        on_device,
        mesh=split,
        in_specs=(rows, rows, rows, P(SIDE), P(SIDE), rows),
        out_specs=(rows, rows, rows, rows),
        check_vma=False,
    )
```

```python
import dataclasses
import functools

import jax
import jax.numpy as jnp
from jax import lax
from jax.experimental import pallas as pl
from jax.experimental.pallas import tpu as pltpu
from jax.sharding import Mesh
from jax.sharding import PartitionSpec as P

BLOCK = 256
LINE = ("ctx_0", "ctx_1")
SIDE = ("row", "core")
EPSILON = 1e-06
GRANT = 12 << 20
F32 = jnp.float32
BF16 = jnp.bfloat16
SMEM = pl.BlockSpec(memory_space=pltpu.SMEM)
VMEM = pl.BlockSpec(memory_space=pltpu.VMEM)


def dot(left, right, left_dim, right_dim):
    return lax.dot_general(
        left, right, (((left_dim,), (right_dim,)), ((), ())), preferred_element_type=F32
    )


def halves(wide):
    high = wide.astype(BF16)
    return high, (wide - high.astype(F32)).astype(BF16)


def dot_wide_right(left, right, left_dim, right_dim):
    high, low = halves(right)
    return dot(left, high, left_dim, right_dim) + dot(left, low, left_dim, right_dim)


def dot_wide_left(left, right, left_dim, right_dim):
    high, low = halves(left)
    return dot(high, right, left_dim, right_dim) + dot(low, right, left_dim, right_dim)


def rows_of(shape):
    return lax.broadcasted_iota(jnp.int32, shape, 0).astype(F32)


def decay_weights(rate):
    shape = (BLOCK, BLOCK)
    spacing = rows_of(shape) - lax.broadcasted_iota(jnp.int32, shape, 1).astype(F32)
    return jnp.where(spacing >= 0, jnp.exp(-rate * jnp.maximum(spacing, 0.0)), 0.0)


def block_rows(block):
    return slice(block * BLOCK, (block + 1) * BLOCK)


@dataclasses.dataclass
class Streamed:
    array: object


@dataclasses.dataclass
class Far:
    array: object


def cols_of(head):
    return slice(head * 128, (head + 1) * 128)


def memory_kernel(rates, keys, values, end, first):
    block = pl.program_id(0)
    to_last = BLOCK - 1.0 - rows_of((BLOCK, 128))
    for head in range(4):
        cols = cols_of(head)
        wide = keys[:, cols].astype(F32) * jnp.exp(-rates[head] * to_last)
        update = dot_wide_left(wide, values[:, cols], 0, 0)
        full = jnp.exp(jnp.full((128, 128), -BLOCK * rates[head], F32))

        @pl.when(block == 0)
        def _():
            first[head] = update

        @pl.when(block > 0)
        def _():
            end[head] = full * first[head] + update


def rate_row(table, head):
    return table[1 + head : 2 + head, 0:128]


def inside_kernel(rates, queries, keys, values, gain, probs, inside, table):
    table[0:1, :] = gain[...]
    for head in range(4):
        table[1 + head : 2 + head, :] = jnp.full((1, table.shape[1]), rates[head], F32)
    for head in range(4):
        cols = cols_of(head)
        weights = decay_weights(rates[head])
        for block in range(2):
            rows = block_rows(block)
            scores = dot(queries[rows, cols], keys[rows, cols], 1, 1)
            low = (scores * weights).astype(BF16)
            probs[head, block] = low
            inside[rows, cols] = dot(low, values[rows, cols], 1, 0)


def carried_kernel(
    table, queries, entering, first, far_inside, out_grad, attention, sums, inside, ready
):
    loads = []
    for block in range(2):
        rows = block_rows(block)
        load = pltpu.make_async_copy(
            far_inside.at[rows, :], inside.at[rows, :], ready.at[block]
        )
        load.start()
        loads.append(load)
    after_start = rows_of((BLOCK, 128)) + 1.0
    squares, products = [], []
    for block in range(2):
        rows = block_rows(block)
        for head in range(4):
            cols = cols_of(head)
            memory = entering[head]
            if block == 1:
                memory = jnp.exp(-BLOCK * rate_row(table, head)) * memory + first[head]
            leading = jnp.exp(-rate_row(table, head) * after_start)
            carried = dot_wide_right(queries[rows, cols], memory, 1, 0)
            attention[rows, cols] = carried * leading
        loads[block].wait()
        square = product = None
        for head in range(4):
            cols = cols_of(head)
            out = inside[rows, cols] + attention[rows, cols]
            attention[rows, cols] = out
            grad = out_grad[rows, cols].astype(F32) * table[0:1, cols]
            square = out * out if square is None else square + out * out
            product = grad * out if product is None else product + grad * out
        for part, flat in ((square, squares), (product, products)):
            for tile in range(2):
                turned = part[tile * 128 : (tile + 1) * 128, :].T
                flat.append(jnp.sum(turned, axis=0, keepdims=True))
    sums[...] = jnp.concatenate(squares + products, axis=0)


def per_token(row):
    return jnp.broadcast_to(row, (128, 128)).T


def scales_of(features, sums, block):
    scale = lax.rsqrt(sums[0:4] / features + EPSILON)
    coeff = scale * sums[4:8] / features
    tiles = (2 * block, 2 * block + 1)
    return tuple(
        jnp.concatenate([per_token(part[tile : tile + 1]) for tile in tiles], axis=0)
        for part in (scale, coeff)
    )


def attention_grad(attention, out_grad, gain, scale, coeff):
    normed = attention * scale
    grad = out_grad.astype(F32) * gain
    return normed, (scale * (grad - normed * coeff)).astype(BF16)


def grad_kernel(features, table, sums, queries, attention, out_grad, end):
    from_start = rows_of((BLOCK, 128))
    for block in (1, 0):
        rows = block_rows(block)
        scale, coeff = scales_of(features, sums, block)
        for head in range(4):
            cols = cols_of(head)
            _, low = attention_grad(
                attention[rows, cols], out_grad[rows, cols], table[0:1, cols], scale, coeff
            )
            start = jnp.exp(-rate_row(table, head) * from_start)
            gathered = dot_wide_left(queries[rows, cols].astype(F32) * start, low, 0, 0)
            if block == 1:
                end[head] = gathered
            else:
                end[head] = jnp.exp(-BLOCK * rate_row(table, head)) * end[head] + gathered


def local_kernel(
    features,
    rates,
    queries,
    keys,
    values,
    out_grad,
    probs,
    entering,
    first,
    sums,
    attention,
    gain,
    query_grad,
    normed_out,
    key_part,
    value_part,
    second,
):
    after_start = rows_of((BLOCK, 128)) + 1.0
    for block in range(2):
        rows = block_rows(block)
        scale, coeff = scales_of(features, sums, block)
        for head in range(4):
            cols = cols_of(head)
            weights = decay_weights(rates[head])
            memory = entering[head]
            if block == 1:
                full = jnp.exp(jnp.full((128, 128), -BLOCK * rates[head], F32))
                memory = full * memory + first[head]
            leading = jnp.exp(-rates[head] * after_start)
            normed, grad = attention_grad(
                attention[rows, cols], out_grad[rows, cols], gain[:, cols], scale, coeff
            )
            normed_out[rows, cols] = (normed * gain[:, cols]).astype(BF16)
            low = (dot(grad, values[rows, cols], 1, 1) * weights).astype(BF16)
            carried = dot_wide_right(grad, memory, 1, 1) * leading
            query_grad[rows, cols] = (dot(low, keys[rows, cols], 1, 0) + carried).astype(BF16)
            key_part[rows, cols] = dot(low, queries[rows, cols], 0, 0)
            value_part[rows, cols] = dot(probs[head, block], grad, 0, 0)
            if block == 1:
                start = jnp.exp(-rates[head] * (after_start - 1.0))
                second[head] = dot_wide_left(queries[rows, cols].astype(F32) * start, grad, 0, 0)


def finish_kernel(
    rates, keys, values, key_part, value_part, after, second, key_grad, value_grad
):
    tile = pl.program_id(0)
    rows = pl.ds(tile * 128, 128)
    to_end = BLOCK - rows_of((128, 128)) - 128.0 * (tile % 2).astype(F32)
    for head in range(4):
        cols = cols_of(head)
        ending = jnp.exp(-rates[head] * to_end)
        full = jnp.exp(jnp.full((128, 128), -BLOCK * rates[head], F32))
        backlog = jnp.where(tile < 2, full * after[head] + second[head], after[head])
        key_more = dot_wide_right(values[rows, cols], backlog, 1, 1) * ending
        value_more = dot_wide_right(keys[rows, cols], backlog, 1, 0) * ending
        key_grad[:, cols] = (key_part[:, cols] + key_more).astype(BF16)
        value_grad[:, cols] = (value_part[:, cols] + value_more).astype(BF16)


def shape(*dims, dtype=F32):
    return jax.ShapeDtypeStruct(dims, dtype)


def near(array):
    return pltpu.with_memory_space_constraint(array, pltpu.VMEM)


def place_of(item):
    if isinstance(item, Far):
        return pl.BlockSpec(memory_space=pltpu.HBM)
    return pl.BlockSpec() if isinstance(item, Streamed) else VMEM


def bare(item):
    return item.array if isinstance(item, (Far, Streamed)) else item


def call(kernel, name, outs, *operands, grant=GRANT, rates=None, scratch=()):
    small = [] if rates is None else [rates]
    return pl.pallas_call(
        kernel,
        in_specs=[SMEM] * len(small) + [place_of(item) for item in operands],
        out_specs=tuple(place_of(item) for item in outs),
        out_shape=tuple(bare(item) for item in outs),
        scratch_shapes=scratch,
        name=name,
        cost_estimate=pl.CostEstimate(
            flops=400_000_000, bytes_accessed=4_000_000, transcendentals=300_000
        ),
        compiler_params=pltpu.CompilerParams(vmem_limit_bytes=grant),
    )(*small, *map(bare, operands))


def scan_total(table, pieces, reverse):
    count, rows, lanes = pieces.shape

    def kernel(table_ref, piece_ref, total_ref):
        order = range(count - 1, -1, -1) if reverse else range(count)
        running = None
        for k in order:
            piece = piece_ref[k]
            running = piece if running is None else running * table_ref[0] + piece
        for peer in range(total_ref.shape[0]):
            total_ref[peer] = running

    return pl.pallas_call(
        kernel,
        in_specs=[SMEM, VMEM],
        out_specs=VMEM,
        out_shape=pltpu.VMEM((lax.axis_size(LINE[0]), rows, lanes), F32),
        name="scan_total",
        compiler_params=pltpu.CompilerParams(vmem_limit_bytes=GRANT),
    )(table, near(pieces))


def scan_prefix(table, pieces, totals, reverse):
    count, rows, lanes = pieces.shape
    first = 5 if reverse else 1

    def kernel(table_ref, piece_ref, total_ref, prefix_ref):
        order = list(range(count - 1, -1, -1) if reverse else range(count))
        running = total_ref[0] * table_ref[first]
        for peer in range(1, total_ref.shape[0]):
            running = running + total_ref[peer] * table_ref[first + peer]
        for k in order:
            prefix_ref[k] = running
            if k != order[-1]:
                running = running * table_ref[0] + piece_ref[k]

    return pl.pallas_call(
        kernel,
        in_specs=[SMEM, VMEM, VMEM],
        out_specs=VMEM,
        out_shape=pltpu.VMEM((count, rows, lanes), F32),
        name="scan_prefix",
        compiler_params=pltpu.CompilerParams(vmem_limit_bytes=GRANT),
    )(table, near(pieces), near(totals))


def line_table(decay_rates, token_count):
    far, near = lax.axis_index(LINE[0]), lax.axis_index(LINE[1])
    far_size, near_size = lax.axis_size(LINE[0]), lax.axis_size(LINE[1])
    rate = lax.dynamic_index_in_dim(
        decay_rates, near * decay_rates.shape[0] // near_size, 0, keepdims=False
    )
    slot = jnp.arange(1 + 2 * far_size)
    earlier = far - slot
    later = slot - 1 - far_size - far - 1
    steps = jnp.where(slot > far_size, later, earlier) * near_size
    steps = jnp.where(slot == 0, 1, steps)
    weights = jnp.exp(-rate * token_count * jnp.maximum(steps, 0).astype(F32))
    return jnp.where(steps >= 0, weights, 0.0)


def along_context(table, state, reverse):
    near_size, far_size = lax.axis_size(LINE[1]), lax.axis_size(LINE[0])
    lanes = state.shape[-1]
    pieces = lax.all_to_all(state.reshape(near_size, -1, lanes), LINE[1], 0, 0)
    totals = lax.all_to_all(scan_total(table, pieces, reverse), LINE[0], 0, 0)
    prefix = scan_prefix(table, pieces, totals, reverse)
    return lax.all_to_all(prefix, LINE[1], 0, 0).reshape(state.shape)


def on_device(queries, key_rows, value_rows, decay_rates, norm_gain, out_grad):
    tokens, width = queries.shape
    heads = decay_rates.shape[0]
    features = float(width * lax.axis_size(SIDE))
    gain = norm_gain[None, :]
    table = line_table(decay_rates, tokens)
    state = shape(heads, 128, 128)
    wide, narrow = shape(tokens, width), shape(tokens, width, dtype=BF16)
    tables = shape(heads, 2, BLOCK, BLOCK, dtype=BF16)
    state_near, wide_near = pltpu.VMEM(state.shape, F32), pltpu.VMEM(wide.shape, F32)
    far_q, far_k, far_v, far_grad = map(Streamed, (queries, key_rows, value_rows, out_grad))
    block_rows_spec = pl.BlockSpec((BLOCK, width), lambda block: (block, 0))
    states = pl.BlockSpec(state.shape, lambda block: (0, 0, 0))
    memory_end, memory_first = pl.pallas_call(
        memory_kernel,
        grid=(tokens // BLOCK,),
        in_specs=[SMEM, block_rows_spec, block_rows_spec],
        out_specs=(states, states),
        out_shape=(state, state),
        name="memory",
    )(decay_rates, key_rows, value_rows)
    probs, inside, aux = call(
        inside_kernel,
        "inside",
        (Streamed(tables), Streamed(wide), pltpu.VMEM((8, width), F32)),
        far_q,
        far_k,
        far_v,
        Streamed(gain),
        grant=None,
        rates=decay_rates,
    )
    entering = along_context(table, memory_end, False)
    attention, sums = call(
        carried_kernel,
        "carried",
        (wide_near, pltpu.VMEM((8, 128), F32)),
        near(aux),
        near(queries),
        near(entering),
        near(memory_first),
        Far(inside),
        near(out_grad),
        grant=None,
        scratch=(wide_near, pltpu.SemaphoreType.DMA((2,))),
    )
    sums = lax.psum(lax.psum(sums, "core"), "row")
    (backlog_end,) = call(
        functools.partial(grad_kernel, features),
        "grad",
        (state_near,),
        near(aux),
        near(sums),
        near(queries),
        near(attention),
        near(out_grad),
    )
    query_grad, normed_out, key_part, value_part, backlog_second = call(
        functools.partial(local_kernel, features),
        "local",
        (Streamed(narrow), Streamed(narrow), Streamed(wide), Streamed(wide), state_near),
        far_q,
        far_k,
        far_v,
        far_grad,
        Streamed(probs),
        near(entering),
        near(memory_first),
        near(sums),
        near(attention),
        Streamed(gain),
        grant=None,
        rates=decay_rates,
    )
    after = along_context(table, backlog_end, True)
    tile_rows = pl.BlockSpec((128, width), lambda tile: (tile, 0))
    key_grad, value_grad = pl.pallas_call(
        finish_kernel,
        grid=(tokens // 128,),
        in_specs=[SMEM] + [VMEM] * 2 + [tile_rows] * 2 + [VMEM] * 2,
        out_specs=(tile_rows, tile_rows),
        out_shape=(narrow, narrow),
        name="finish",
    )(
        decay_rates,
        near(key_rows),
        near(value_rows),
        key_part,
        value_part,
        near(after),
        near(backlog_second),
    )
    return (normed_out, query_grad, key_grad, value_grad)


def solution(mesh):
    split = Mesh(mesh.devices.reshape(4, 16, 4, 2), LINE + SIDE)
    rows = P(LINE, SIDE)
    return jax.shard_map(
        on_device,
        mesh=split,
        in_specs=(rows, rows, rows, P(SIDE), P(SIDE), rows),
        out_specs=(rows, rows, rows, rows),
        check_vma=False,
    )
```

```python
import dataclasses
import functools

import jax
import jax.numpy as jnp
from jax import lax
from jax.experimental import pallas as pl
from jax.experimental.pallas import tpu as pltpu
from jax.sharding import Mesh
from jax.sharding import PartitionSpec as P

BLOCK = 256
LINE = ("ctx_0", "ctx_1")
SIDE = ("row", "core")
EPSILON = 1e-06
GRANT = 12 << 20
F32 = jnp.float32
BF16 = jnp.bfloat16
SMEM = pl.BlockSpec(memory_space=pltpu.SMEM)
VMEM = pl.BlockSpec(memory_space=pltpu.VMEM)


def dot(left, right, left_dim, right_dim):
    return lax.dot_general(
        left, right, (((left_dim,), (right_dim,)), ((), ())), preferred_element_type=F32
    )


def halves(wide):
    high = wide.astype(BF16)
    return high, (wide - high.astype(F32)).astype(BF16)


def dot_wide_right(left, right, left_dim, right_dim):
    twice = jnp.concatenate([left, left], axis=left_dim)
    return dot(twice, jnp.concatenate(halves(right), axis=right_dim), left_dim, right_dim)


def dot_wide_left(left, right):
    both = dot(jnp.concatenate(halves(left), axis=1), right, 0, 0)
    width = left.shape[1]
    return both[:width] + both[width:]


def rows_of(shape):
    return lax.broadcasted_iota(jnp.int32, shape, 0).astype(F32)


def decay_weights(rate):
    shape = (BLOCK, BLOCK)
    spacing = rows_of(shape) - lax.broadcasted_iota(jnp.int32, shape, 1).astype(F32)
    return jnp.where(spacing >= 0, jnp.exp(-rate * jnp.maximum(spacing, 0.0)), 0.0)


def block_rows(block):
    return slice(block * BLOCK, (block + 1) * BLOCK)


@dataclasses.dataclass
class Streamed:
    array: object


@dataclasses.dataclass
class Far:
    array: object


def cols_of(head):
    return slice(head * 128, (head + 1) * 128)


def start_copies(pairs, flags):
    copies = []
    for source, target in pairs:
        copy = pltpu.make_async_copy(source, target, flags.at[len(copies)])
        copy.start()
        copies.append(copy)
    return copies


def wait_all(copies):
    for copy in copies:
        copy.wait()


def memory_kernel(rates, far_keys, far_values, end, first, keys, values, ready):
    loads = []
    for block in range(2):
        rows = block_rows(block)
        pairs = ((far_keys, keys), (far_values, values))
        loads.append(
            start_copies([(f.at[rows, :], n.at[rows, :]) for f, n in pairs], ready.at[block])
        )
    to_last = BLOCK - 1.0 - rows_of((BLOCK, 128))
    for block in range(2):
        rows = block_rows(block)
        wait_all(loads[block])
        for head in range(4):
            cols = cols_of(head)
            wide = keys[rows, cols].astype(F32) * jnp.exp(-rates[head] * to_last)
            update = dot_wide_left(wide, values[rows, cols])
            if block == 0:
                first[head] = update
            else:
                full = jnp.exp(jnp.full((128, 128), -BLOCK * rates[head], F32))
                end[head] = full * first[head] + update


def rate_row(table, head):
    return table[1 + head : 2 + head, 0:128]


def inside_kernel(rates, queries, keys, values, gain, probs, inside, table):
    table[0:1, :] = gain[...]
    for head in range(4):
        table[1 + head : 2 + head, :] = jnp.full((1, table.shape[1]), rates[head], F32)
    for head in range(4):
        cols = cols_of(head)
        weights = decay_weights(rates[head])
        for block in range(2):
            rows = block_rows(block)
            scores = dot(queries[rows, cols], keys[rows, cols], 1, 1)
            low = (scores * weights).astype(BF16)
            probs[head, block] = low
            inside[rows, cols] = dot(low, values[rows, cols], 1, 0)


def carried_kernel(
    table, queries, entering, first, far_inside, out_grad, attention, sums, inside, ready
):
    loads = []
    for block in range(2):
        rows = block_rows(block)
        load = pltpu.make_async_copy(
            far_inside.at[rows, :], inside.at[rows, :], ready.at[block]
        )
        load.start()
        loads.append(load)
    after_start = rows_of((BLOCK, 128)) + 1.0
    squares, products = [], []
    for block in range(2):
        rows = block_rows(block)
        for head in range(4):
            cols = cols_of(head)
            memory = entering[head]
            if block == 1:
                memory = jnp.exp(-BLOCK * rate_row(table, head)) * memory + first[head]
            leading = jnp.exp(-rate_row(table, head) * after_start)
            carried = dot_wide_right(queries[rows, cols], memory, 1, 0)
            attention[rows, cols] = carried * leading
        loads[block].wait()
        square = product = None
        for head in range(4):
            cols = cols_of(head)
            out = inside[rows, cols] + attention[rows, cols]
            attention[rows, cols] = out
            grad = out_grad[rows, cols].astype(F32) * table[0:1, cols]
            square = out * out if square is None else square + out * out
            product = grad * out if product is None else product + grad * out
        for part, flat in ((square, squares), (product, products)):
            for tile in range(2):
                turned = part[tile * 128 : (tile + 1) * 128, :].T
                flat.append(jnp.sum(turned, axis=0, keepdims=True))
    sums[...] = jnp.concatenate(squares + products, axis=0)


def per_token(row):
    return jnp.broadcast_to(row, (128, 128)).T


def scales_of(features, sums, block):
    scale = lax.rsqrt(sums[0:4] / features + EPSILON)
    coeff = scale * sums[4:8] / features
    tiles = (2 * block, 2 * block + 1)
    return tuple(
        jnp.concatenate([per_token(part[tile : tile + 1]) for tile in tiles], axis=0)
        for part in (scale, coeff)
    )


def attention_grad(attention, out_grad, gain, scale, coeff):
    normed = attention * scale
    grad = out_grad.astype(F32) * gain
    return normed, (scale * (grad - normed * coeff)).astype(BF16)


def grad_kernel(features, table, sums, queries, attention, out_grad, end):
    from_start = rows_of((BLOCK, 128))
    for block in (1, 0):
        rows = block_rows(block)
        scale, coeff = scales_of(features, sums, block)
        for head in range(4):
            cols = cols_of(head)
            _, low = attention_grad(
                attention[rows, cols], out_grad[rows, cols], table[0:1, cols], scale, coeff
            )
            start = jnp.exp(-rate_row(table, head) * from_start)
            gathered = dot_wide_left(queries[rows, cols].astype(F32) * start, low)
            if block == 1:
                end[head] = gathered
            else:
                end[head] = jnp.exp(-BLOCK * rate_row(table, head)) * end[head] + gathered


def local_kernel(
    features,
    rates,
    queries,
    keys,
    values,
    out_grad,
    probs,
    entering,
    first,
    sums,
    attention,
    gain,
    query_grad,
    normed_out,
    key_part,
    value_part,
    second,
):
    after_start = rows_of((BLOCK, 128)) + 1.0
    for block in range(2):
        rows = block_rows(block)
        scale, coeff = scales_of(features, sums, block)
        for head in range(4):
            cols = cols_of(head)
            weights = decay_weights(rates[head])
            memory = entering[head]
            if block == 1:
                full = jnp.exp(jnp.full((128, 128), -BLOCK * rates[head], F32))
                memory = full * memory + first[head]
            leading = jnp.exp(-rates[head] * after_start)
            normed, grad = attention_grad(
                attention[rows, cols], out_grad[rows, cols], gain[:, cols], scale, coeff
            )
            normed_out[rows, cols] = (normed * gain[:, cols]).astype(BF16)
            low = (dot(grad, values[rows, cols], 1, 1) * weights).astype(BF16)
            carried = dot_wide_right(grad, memory, 1, 1) * leading
            query_grad[rows, cols] = (dot(low, keys[rows, cols], 1, 0) + carried).astype(BF16)
            key_part[rows, cols] = dot(low, queries[rows, cols], 0, 0)
            value_part[rows, cols] = dot(probs[head, block], grad, 0, 0)
            if block == 1:
                start = jnp.exp(-rates[head] * (after_start - 1.0))
                second[head] = dot_wide_left(queries[rows, cols].astype(F32) * start, grad)


def finish_kernel(
    rates,
    keys,
    values,
    far_key_part,
    far_value_part,
    after,
    second,
    far_key_grad,
    far_value_grad,
    key_part,
    value_part,
    key_more,
    value_more,
    key_grad,
    value_grad,
    ready,
    done,
):
    loads, stores = [], []
    for block in range(2):
        rows = block_rows(block)
        pairs = ((far_key_part, key_part), (far_value_part, value_part))
        loads.append(
            start_copies([(f.at[rows, :], n.at[rows, :]) for f, n in pairs], ready.at[block])
        )
    to_end = BLOCK - rows_of((BLOCK, 128))
    for block in range(2):
        rows = block_rows(block)
        for head in range(4):
            cols = cols_of(head)
            ending = jnp.exp(-rates[head] * to_end)
            backlog = after[head]
            if block == 0:
                full = jnp.exp(jnp.full((128, 128), -BLOCK * rates[head], F32))
                backlog = full * backlog + second[head]
            key_more[:, cols] = dot_wide_right(values[rows, cols], backlog, 1, 1) * ending
            value_more[:, cols] = dot_wide_right(keys[rows, cols], backlog, 1, 0) * ending
        wait_all(loads[block])
        key_grad[rows, :] = (key_part[rows, :] + key_more[...]).astype(BF16)
        value_grad[rows, :] = (value_part[rows, :] + value_more[...]).astype(BF16)
        pairs = ((key_grad, far_key_grad), (value_grad, far_value_grad))
        stores += start_copies([(n.at[rows, :], f.at[rows, :]) for n, f in pairs], done.at[block])
    wait_all(stores)


def shape(*dims, dtype=F32):
    return jax.ShapeDtypeStruct(dims, dtype)


def near(array):
    return pltpu.with_memory_space_constraint(array, pltpu.VMEM)


def place_of(item):
    if isinstance(item, Far):
        return pl.BlockSpec(memory_space=pltpu.HBM)
    return pl.BlockSpec() if isinstance(item, Streamed) else VMEM


def bare(item):
    return item.array if isinstance(item, (Far, Streamed)) else item


def call(kernel, name, outs, *operands, grant=GRANT, rates=None, scratch=()):
    small = [] if rates is None else [rates]
    return pl.pallas_call(
        kernel,
        in_specs=[SMEM] * len(small) + [place_of(item) for item in operands],
        out_specs=tuple(place_of(item) for item in outs),
        out_shape=tuple(bare(item) for item in outs),
        scratch_shapes=scratch,
        name=name,
        cost_estimate=pl.CostEstimate(
            flops=400_000_000, bytes_accessed=4_000_000, transcendentals=300_000
        ),
        compiler_params=pltpu.CompilerParams(vmem_limit_bytes=grant),
    )(*small, *map(bare, operands))


def scan_total(table, pieces, reverse):
    count, rows, lanes = pieces.shape

    def kernel(table_ref, piece_ref, total_ref):
        order = range(count - 1, -1, -1) if reverse else range(count)
        running = None
        for k in order:
            piece = piece_ref[k]
            running = piece if running is None else running * table_ref[0] + piece
        for peer in range(total_ref.shape[0]):
            total_ref[peer] = running

    return pl.pallas_call(
        kernel,
        in_specs=[SMEM, VMEM],
        out_specs=VMEM,
        out_shape=pltpu.VMEM((lax.axis_size(LINE[0]), rows, lanes), F32),
        name="scan_total",
        compiler_params=pltpu.CompilerParams(vmem_limit_bytes=GRANT),
    )(table, near(pieces))


def scan_prefix(table, pieces, totals, reverse):
    count, rows, lanes = pieces.shape
    first = 5 if reverse else 1
    stride = count // 4

    def kernel(table_ref, piece_ref, total_ref, far_ref, prefix_ref, done):
        running = total_ref[0] * table_ref[first]
        for peer in range(1, total_ref.shape[0]):
            running = running + total_ref[peer] * table_ref[first + peer]
        stores = []
        for part in range(4):
            order = range(part * stride, (part + 1) * stride)
            for step in order:
                k = count - 1 - step if reverse else step
                prefix_ref[k] = running
                if step != count - 1:
                    running = running * table_ref[0] + piece_ref[k]
            low = count - (part + 1) * stride if reverse else part * stride
            span = slice(low, low + stride)
            store = pltpu.make_async_copy(prefix_ref.at[span], far_ref.at[span], done.at[part])
            store.start()
            stores.append(store)
        wait_all(stores)

    return pl.pallas_call(
        kernel,
        in_specs=[SMEM, VMEM, VMEM],
        out_specs=pl.BlockSpec(memory_space=pltpu.HBM),
        out_shape=shape(count, rows, lanes),
        scratch_shapes=(pltpu.VMEM((count, rows, lanes), F32), pltpu.SemaphoreType.DMA((4,))),
        name="scan_prefix",
        compiler_params=pltpu.CompilerParams(vmem_limit_bytes=GRANT),
    )(table, near(pieces), near(totals))


def line_table(decay_rates, token_count):
    far, near = lax.axis_index(LINE[0]), lax.axis_index(LINE[1])
    far_size, near_size = lax.axis_size(LINE[0]), lax.axis_size(LINE[1])
    rate = lax.dynamic_index_in_dim(
        decay_rates, near * decay_rates.shape[0] // near_size, 0, keepdims=False
    )
    slot = jnp.arange(1 + 2 * far_size)
    earlier = far - slot
    later = slot - 1 - far_size - far - 1
    steps = jnp.where(slot > far_size, later, earlier) * near_size
    steps = jnp.where(slot == 0, 1, steps)
    weights = jnp.exp(-rate * token_count * jnp.maximum(steps, 0).astype(F32))
    return jnp.where(steps >= 0, weights, 0.0)


def along_context(table, state, reverse):
    near_size, far_size = lax.axis_size(LINE[1]), lax.axis_size(LINE[0])
    lanes = state.shape[-1]
    pieces = lax.all_to_all(state.reshape(near_size, -1, lanes), LINE[1], 0, 0)
    totals = lax.all_to_all(scan_total(table, pieces, reverse), LINE[0], 0, 0)
    prefix = scan_prefix(table, pieces, totals, reverse)
    return lax.all_to_all(prefix, LINE[1], 0, 0).reshape(state.shape)


def on_device(queries, key_rows, value_rows, decay_rates, norm_gain, out_grad):
    tokens, width = queries.shape
    heads = decay_rates.shape[0]
    features = float(width * lax.axis_size(SIDE))
    gain = norm_gain[None, :]
    table = line_table(decay_rates, tokens)
    state = shape(heads, 128, 128)
    wide, narrow = shape(tokens, width), shape(tokens, width, dtype=BF16)
    tables = shape(heads, 2, BLOCK, BLOCK, dtype=BF16)
    state_near, wide_near = pltpu.VMEM(state.shape, F32), pltpu.VMEM(wide.shape, F32)
    far_q, far_k, far_v, far_grad = map(Streamed, (queries, key_rows, value_rows, out_grad))
    narrow_near, flags = pltpu.VMEM(narrow.shape, BF16), pltpu.SemaphoreType.DMA((2, 2))
    memory_end, memory_first = call(
        memory_kernel,
        "memory",
        (Streamed(state), state_near),
        Far(key_rows),
        Far(value_rows),
        grant=None,
        rates=decay_rates,
        scratch=(narrow_near, narrow_near, flags),
    )
    probs, inside, aux = call(
        inside_kernel,
        "inside",
        (Streamed(tables), Streamed(wide), pltpu.VMEM((8, width), F32)),
        far_q,
        far_k,
        far_v,
        Streamed(gain),
        grant=None,
        rates=decay_rates,
    )
    entering = along_context(table, memory_end, False)
    attention, sums = call(
        carried_kernel,
        "carried",
        (wide_near, pltpu.VMEM((8, 128), F32)),
        near(aux),
        near(queries),
        near(entering),
        near(memory_first),
        Far(inside),
        near(out_grad),
        grant=None,
        scratch=(wide_near, pltpu.SemaphoreType.DMA((2,))),
    )
    sums = lax.psum(lax.psum(sums, "core"), "row")
    (backlog_end,) = call(
        functools.partial(grad_kernel, features),
        "grad",
        (state_near,),
        near(aux),
        near(sums),
        near(queries),
        near(attention),
        near(out_grad),
    )
    query_grad, normed_out, key_part, value_part, backlog_second = call(
        functools.partial(local_kernel, features),
        "local",
        (Streamed(narrow), Streamed(narrow), Streamed(wide), Streamed(wide), state_near),
        far_q,
        far_k,
        far_v,
        far_grad,
        Streamed(probs),
        near(entering),
        near(memory_first),
        near(sums),
        near(attention),
        Streamed(gain),
        grant=None,
        rates=decay_rates,
    )
    after = along_context(table, backlog_end, True)
    more = pltpu.VMEM((BLOCK, width), F32)
    key_grad, value_grad = call(
        finish_kernel,
        "finish",
        (Far(narrow), Far(narrow)),
        near(key_rows),
        near(value_rows),
        Far(key_part),
        Far(value_part),
        near(after),
        near(backlog_second),
        grant=None,
        rates=decay_rates,
        scratch=(wide_near, wide_near, more, more, narrow_near, narrow_near, flags, flags),
    )
    return (normed_out, query_grad, key_grad, value_grad)


def solution(mesh):
    split = Mesh(mesh.devices.reshape(4, 16, 4, 2), LINE + SIDE)
    rows = P(LINE, SIDE)
    return jax.shard_map(
        on_device,
        mesh=split,
        in_specs=(rows, rows, rows, P(SIDE), P(SIDE), rows),
        out_specs=(rows, rows, rows, rows),
        check_vma=False,
    )
```

```python
import dataclasses
import functools

import jax
import jax.numpy as jnp
from jax import lax
from jax.experimental import pallas as pl
from jax.experimental.pallas import tpu as pltpu
from jax.sharding import Mesh
from jax.sharding import PartitionSpec as P

BLOCK = 256
LINE = ("ctx_0", "ctx_1")
SIDE = ("row", "core")
EPSILON = 1e-06
GRANT = 12 << 20
F32 = jnp.float32
BF16 = jnp.bfloat16
SMEM = pl.BlockSpec(memory_space=pltpu.SMEM)
VMEM = pl.BlockSpec(memory_space=pltpu.VMEM)


def dot(left, right, left_dim, right_dim):
    return lax.dot_general(
        left, right, (((left_dim,), (right_dim,)), ((), ())), preferred_element_type=F32
    )


def halves(wide):
    high = wide.astype(BF16)
    return high, (wide - high.astype(F32)).astype(BF16)


def dot_wide_right(left, right, left_dim, right_dim):
    twice = jnp.concatenate([left, left], axis=left_dim)
    return dot(twice, jnp.concatenate(halves(right), axis=right_dim), left_dim, right_dim)


def dot_wide_left(left, right):
    both = dot(jnp.concatenate(halves(left), axis=1), right, 0, 0)
    width = left.shape[1]
    return both[:width] + both[width:]


def rows_of(shape):
    return lax.broadcasted_iota(jnp.int32, shape, 0).astype(F32)


def decay_weights(rate):
    shape = (BLOCK, BLOCK)
    spacing = rows_of(shape) - lax.broadcasted_iota(jnp.int32, shape, 1).astype(F32)
    return jnp.where(spacing >= 0, jnp.exp(-rate * jnp.maximum(spacing, 0.0)), 0.0)


def block_rows(block):
    return slice(block * BLOCK, (block + 1) * BLOCK)


@dataclasses.dataclass
class Streamed:
    array: object


@dataclasses.dataclass
class Far:
    array: object


def cols_of(head):
    return slice(head * 128, (head + 1) * 128)


def start_copies(pairs, flags):
    copies = []
    for source, target in pairs:
        copy = pltpu.make_async_copy(source, target, flags.at[len(copies)])
        copy.start()
        copies.append(copy)
    return copies


def wait_all(copies):
    for copy in copies:
        copy.wait()


def memory_kernel(
    rates, far_keys, far_values, far_end, first, keys, values, end, ready, done
):
    stores = []
    loads = []
    for block in range(2):
        rows = block_rows(block)
        pairs = ((far_keys, keys), (far_values, values))
        loads.append(
            start_copies([(f.at[rows, :], n.at[rows, :]) for f, n in pairs], ready.at[block])
        )
    to_last = BLOCK - 1.0 - rows_of((BLOCK, 128))
    for block in range(2):
        rows = block_rows(block)
        wait_all(loads[block])
        for head in range(4):
            cols = cols_of(head)
            wide = keys[rows, cols].astype(F32) * jnp.exp(-rates[head] * to_last)
            update = dot_wide_left(wide, values[rows, cols])
            if block == 0:
                first[head] = update
            else:
                full = jnp.exp(jnp.full((128, 128), -BLOCK * rates[head], F32))
                end[head] = full * first[head] + update
                store = pltpu.make_async_copy(end.at[head], far_end.at[head], done.at[head])
                store.start()
                stores.append(store)
    wait_all(stores)


def rate_row(table, head):
    return table[1 + head : 2 + head, 0:128]


def inside_kernel(rates, queries, keys, values, gain, probs, inside, table):
    table[0:1, :] = gain[...]
    for head in range(4):
        table[1 + head : 2 + head, :] = jnp.full((1, table.shape[1]), rates[head], F32)
    for head in range(4):
        cols = cols_of(head)
        weights = decay_weights(rates[head])
        for block in range(2):
            rows = block_rows(block)
            scores = dot(queries[rows, cols], keys[rows, cols], 1, 1)
            low = (scores * weights).astype(BF16)
            probs[head, block] = low
            inside[rows, cols] = dot(low, values[rows, cols], 1, 0)


def carried_kernel(
    table, queries, entering, first, far_inside, out_grad, attention, sums, inside, ready
):
    loads = []
    for block in range(2):
        rows = block_rows(block)
        load = pltpu.make_async_copy(
            far_inside.at[rows, :], inside.at[rows, :], ready.at[block]
        )
        load.start()
        loads.append(load)
    after_start = rows_of((BLOCK, 128)) + 1.0
    squares, products = [], []
    for block in range(2):
        rows = block_rows(block)
        for head in range(4):
            cols = cols_of(head)
            memory = entering[head]
            if block == 1:
                memory = jnp.exp(-BLOCK * rate_row(table, head)) * memory + first[head]
            leading = jnp.exp(-rate_row(table, head) * after_start)
            carried = dot_wide_right(queries[rows, cols], memory, 1, 0)
            attention[rows, cols] = carried * leading
        loads[block].wait()
        square = product = None
        for head in range(4):
            cols = cols_of(head)
            out = inside[rows, cols] + attention[rows, cols]
            attention[rows, cols] = out
            grad = out_grad[rows, cols].astype(F32) * table[0:1, cols]
            square = out * out if square is None else square + out * out
            product = grad * out if product is None else product + grad * out
        for part, flat in ((square, squares), (product, products)):
            for tile in range(2):
                turned = part[tile * 128 : (tile + 1) * 128, :].T
                flat.append(jnp.sum(turned, axis=0, keepdims=True))
    sums[...] = jnp.concatenate(squares + products, axis=0)


def per_token(row):
    return jnp.broadcast_to(row, (128, 128)).T


def scales_of(features, sums, block):
    scale = lax.rsqrt(sums[0:4] / features + EPSILON)
    coeff = scale * sums[4:8] / features
    tiles = (2 * block, 2 * block + 1)
    return tuple(
        jnp.concatenate([per_token(part[tile : tile + 1]) for tile in tiles], axis=0)
        for part in (scale, coeff)
    )


def attention_grad(attention, out_grad, gain, scale, coeff):
    normed = attention * scale
    grad = out_grad.astype(F32) * gain
    return normed, (scale * (grad - normed * coeff)).astype(BF16)


def grad_kernel(features, table, sums, queries, attention, out_grad, end):
    from_start = rows_of((BLOCK, 128))
    for block in (1, 0):
        rows = block_rows(block)
        scale, coeff = scales_of(features, sums, block)
        for head in range(4):
            cols = cols_of(head)
            _, low = attention_grad(
                attention[rows, cols], out_grad[rows, cols], table[0:1, cols], scale, coeff
            )
            start = jnp.exp(-rate_row(table, head) * from_start)
            gathered = dot_wide_left(queries[rows, cols].astype(F32) * start, low)
            if block == 1:
                end[head] = gathered
            else:
                end[head] = jnp.exp(-BLOCK * rate_row(table, head)) * end[head] + gathered


def local_kernel(
    features,
    rates,
    queries,
    keys,
    values,
    out_grad,
    probs,
    entering,
    first,
    sums,
    attention,
    gain,
    query_grad,
    normed_out,
    key_part,
    value_part,
    second,
):
    after_start = rows_of((BLOCK, 128)) + 1.0
    for block in range(2):
        rows = block_rows(block)
        scale, coeff = scales_of(features, sums, block)
        for head in range(4):
            cols = cols_of(head)
            weights = decay_weights(rates[head])
            memory = entering[head]
            if block == 1:
                full = jnp.exp(jnp.full((128, 128), -BLOCK * rates[head], F32))
                memory = full * memory + first[head]
            leading = jnp.exp(-rates[head] * after_start)
            normed, grad = attention_grad(
                attention[rows, cols], out_grad[rows, cols], gain[:, cols], scale, coeff
            )
            normed_out[rows, cols] = (normed * gain[:, cols]).astype(BF16)
            low = (dot(grad, values[rows, cols], 1, 1) * weights).astype(BF16)
            carried = dot_wide_right(grad, memory, 1, 1) * leading
            query_grad[rows, cols] = (dot(low, keys[rows, cols], 1, 0) + carried).astype(BF16)
            key_part[rows, cols] = dot(low, queries[rows, cols], 0, 0)
            value_part[rows, cols] = dot(probs[head, block], grad, 0, 0)
            if block == 1:
                start = jnp.exp(-rates[head] * (after_start - 1.0))
                second[head] = dot_wide_left(queries[rows, cols].astype(F32) * start, grad)


def finish_kernel(
    rates,
    keys,
    values,
    far_key_part,
    far_value_part,
    after,
    second,
    far_key_grad,
    far_value_grad,
    key_part,
    value_part,
    key_more,
    value_more,
    key_grad,
    value_grad,
    ready,
    done,
):
    loads, stores = [], []
    for block in range(2):
        rows = block_rows(block)
        pairs = ((far_key_part, key_part), (far_value_part, value_part))
        loads.append(
            start_copies([(f.at[rows, :], n.at[rows, :]) for f, n in pairs], ready.at[block])
        )
    to_end = BLOCK - rows_of((BLOCK, 128))
    for block in range(2):
        rows = block_rows(block)
        for head in range(4):
            cols = cols_of(head)
            ending = jnp.exp(-rates[head] * to_end)
            backlog = after[head]
            if block == 0:
                full = jnp.exp(jnp.full((128, 128), -BLOCK * rates[head], F32))
                backlog = full * backlog + second[head]
            key_more[:, cols] = dot_wide_right(values[rows, cols], backlog, 1, 1) * ending
            value_more[:, cols] = dot_wide_right(keys[rows, cols], backlog, 1, 0) * ending
        wait_all(loads[block])
        for half in range(4):
            span = slice(block * BLOCK + half * 64, block * BLOCK + half * 64 + 64)
            own = slice(half * 64, half * 64 + 64)
            key_grad[span, :] = (key_part[span, :] + key_more[own, :]).astype(BF16)
            value_grad[span, :] = (value_part[span, :] + value_more[own, :]).astype(BF16)
            pairs = ((key_grad, far_key_grad), (value_grad, far_value_grad))
            stores += start_copies(
                [(n.at[span, :], f.at[span, :]) for n, f in pairs], done.at[4 * block + half]
            )
    wait_all(stores)


def shape(*dims, dtype=F32):
    return jax.ShapeDtypeStruct(dims, dtype)


def near(array):
    return pltpu.with_memory_space_constraint(array, pltpu.VMEM)


def place_of(item):
    if isinstance(item, Far):
        return pl.BlockSpec(memory_space=pltpu.HBM)
    return pl.BlockSpec() if isinstance(item, Streamed) else VMEM


def bare(item):
    return item.array if isinstance(item, (Far, Streamed)) else item


def call(kernel, name, outs, *operands, grant=GRANT, rates=None, scratch=()):
    small = [] if rates is None else [rates]
    return pl.pallas_call(
        kernel,
        in_specs=[SMEM] * len(small) + [place_of(item) for item in operands],
        out_specs=tuple(place_of(item) for item in outs),
        out_shape=tuple(bare(item) for item in outs),
        scratch_shapes=scratch,
        name=name,
        cost_estimate=pl.CostEstimate(
            flops=400_000_000, bytes_accessed=4_000_000, transcendentals=300_000
        ),
        compiler_params=pltpu.CompilerParams(vmem_limit_bytes=grant),
    )(*small, *map(bare, operands))


def scan_total(table, pieces, reverse, filled):
    count, rows, lanes = pieces.shape

    def kernel(table_ref, piece_ref, _, total_ref):
        order = range(count - 1, -1, -1) if reverse else range(count)
        running = None
        for k in order:
            piece = piece_ref[k]
            running = piece if running is None else running * table_ref[0] + piece
        for peer in range(total_ref.shape[0]):
            total_ref[peer] = running

    return pl.pallas_call(
        kernel,
        in_specs=[SMEM, VMEM, VMEM],
        out_specs=VMEM,
        out_shape=pltpu.VMEM((lax.axis_size(LINE[0]), rows, lanes), F32),
        name="scan_total",
        compiler_params=pltpu.CompilerParams(vmem_limit_bytes=GRANT),
    )(table, near(pieces), near(filled))


def scan_prefix(table, pieces, totals, reverse):
    count, rows, lanes = pieces.shape
    first = 5 if reverse else 1

    def kernel(table_ref, piece_ref, total_ref, prefix_ref):
        order = list(range(count - 1, -1, -1) if reverse else range(count))
        running = total_ref[0] * table_ref[first]
        for peer in range(1, total_ref.shape[0]):
            running = running + total_ref[peer] * table_ref[first + peer]
        for k in order:
            prefix_ref[k] = running
            if k != order[-1]:
                running = running * table_ref[0] + piece_ref[k]

    return pl.pallas_call(
        kernel,
        in_specs=[SMEM, VMEM, VMEM],
        out_specs=VMEM,
        out_shape=pltpu.VMEM((count, rows, lanes), F32),
        name="scan_prefix",
        compiler_params=pltpu.CompilerParams(vmem_limit_bytes=GRANT),
    )(table, near(pieces), near(totals))


def line_table(decay_rates, token_count):
    far, near = lax.axis_index(LINE[0]), lax.axis_index(LINE[1])
    far_size, near_size = lax.axis_size(LINE[0]), lax.axis_size(LINE[1])
    rate = lax.dynamic_index_in_dim(
        decay_rates, near * decay_rates.shape[0] // near_size, 0, keepdims=False
    )
    slot = jnp.arange(1 + 2 * far_size)
    earlier = far - slot
    later = slot - 1 - far_size - far - 1
    steps = jnp.where(slot > far_size, later, earlier) * near_size
    steps = jnp.where(slot == 0, 1, steps)
    weights = jnp.exp(-rate * token_count * jnp.maximum(steps, 0).astype(F32))
    return jnp.where(steps >= 0, weights, 0.0)


def along_context(table, state, reverse, filled):
    near_size, far_size = lax.axis_size(LINE[1]), lax.axis_size(LINE[0])
    lanes = state.shape[-1]
    pieces = lax.all_to_all(state.reshape(near_size, -1, lanes), LINE[1], 0, 0)
    totals = lax.all_to_all(scan_total(table, pieces, reverse, filled), LINE[0], 0, 0)
    prefix = scan_prefix(table, pieces, totals, reverse)
    return lax.all_to_all(prefix, LINE[1], 0, 0).reshape(state.shape)


def on_device(queries, key_rows, value_rows, decay_rates, norm_gain, out_grad):
    tokens, width = queries.shape
    heads = decay_rates.shape[0]
    features = float(width * lax.axis_size(SIDE))
    gain = norm_gain[None, :]
    table = line_table(decay_rates, tokens)
    state = shape(heads, 128, 128)
    wide, narrow = shape(tokens, width), shape(tokens, width, dtype=BF16)
    tables = shape(heads, 2, BLOCK, BLOCK, dtype=BF16)
    state_near, wide_near = pltpu.VMEM(state.shape, F32), pltpu.VMEM(wide.shape, F32)
    far_q, far_k, far_v, far_grad = map(Streamed, (queries, key_rows, value_rows, out_grad))
    narrow_near, flags = pltpu.VMEM(narrow.shape, BF16), pltpu.SemaphoreType.DMA((2, 2))
    memory_end, memory_first = call(
        memory_kernel,
        "memory",
        (Far(state), state_near),
        Far(key_rows),
        Far(value_rows),
        grant=None,
        rates=decay_rates,
        scratch=(narrow_near, narrow_near, state_near, flags, pltpu.SemaphoreType.DMA((4,))),
    )
    probs, inside, aux = call(
        inside_kernel,
        "inside",
        (Streamed(tables), Streamed(wide), pltpu.VMEM((8, width), F32)),
        far_q,
        far_k,
        far_v,
        Streamed(gain),
        grant=None,
        rates=decay_rates,
    )
    entering = along_context(table, memory_end, False, aux)
    attention, sums = call(
        carried_kernel,
        "carried",
        (wide_near, pltpu.VMEM((8, 128), F32)),
        near(aux),
        near(queries),
        near(entering),
        near(memory_first),
        Far(inside),
        near(out_grad),
        grant=None,
        scratch=(wide_near, pltpu.SemaphoreType.DMA((2,))),
    )
    sums = lax.psum(lax.psum(sums, "core"), "row")
    (backlog_end,) = call(
        functools.partial(grad_kernel, features),
        "grad",
        (state_near,),
        near(aux),
        near(sums),
        near(queries),
        near(attention),
        near(out_grad),
    )
    query_grad, normed_out, key_part, value_part, backlog_second = call(
        functools.partial(local_kernel, features),
        "local",
        (Streamed(narrow), Streamed(narrow), Streamed(wide), Streamed(wide), state_near),
        far_q,
        far_k,
        far_v,
        far_grad,
        Streamed(probs),
        near(entering),
        near(memory_first),
        near(sums),
        near(attention),
        Streamed(gain),
        grant=None,
        rates=decay_rates,
    )
    after = along_context(table, backlog_end, True, backlog_second)
    more = pltpu.VMEM((BLOCK, width), F32)
    key_grad, value_grad = call(
        finish_kernel,
        "finish",
        (Far(narrow), Far(narrow)),
        near(key_rows),
        near(value_rows),
        Far(key_part),
        Far(value_part),
        near(after),
        near(backlog_second),
        grant=None,
        rates=decay_rates,
        scratch=(wide_near, wide_near, more, more, narrow_near, narrow_near, flags, pltpu.SemaphoreType.DMA((8, 2))),
    )
    return (normed_out, query_grad, key_grad, value_grad)


def solution(mesh):
    split = Mesh(mesh.devices.reshape(4, 16, 4, 2), LINE + SIDE)
    rows = P(LINE, SIDE)
    return jax.shard_map(
        on_device,
        mesh=split,
        in_specs=(rows, rows, rows, P(SIDE), P(SIDE), rows),
        out_specs=(rows, rows, rows, rows),
        check_vma=False,
    )
```

```python
import dataclasses
import functools

import jax
import jax.numpy as jnp
from jax import lax
from jax.experimental import pallas as pl
from jax.experimental.pallas import tpu as pltpu
from jax.sharding import Mesh
from jax.sharding import PartitionSpec as P

BLOCK = 256
LINE = ("ctx_0", "ctx_1")
SIDE = ("row", "core")
EPSILON = 1e-06
GRANT = 12 << 20
F32 = jnp.float32
BF16 = jnp.bfloat16
SMEM = pl.BlockSpec(memory_space=pltpu.SMEM)
VMEM = pl.BlockSpec(memory_space=pltpu.VMEM)


def dot(left, right, left_dim, right_dim):
    return lax.dot_general(
        left, right, (((left_dim,), (right_dim,)), ((), ())), preferred_element_type=F32
    )


def halves(wide):
    high = wide.astype(BF16)
    return high, (wide - high.astype(F32)).astype(BF16)


def dot_wide_right(left, right, left_dim, right_dim):
    twice = jnp.concatenate([left, left], axis=left_dim)
    return dot(twice, jnp.concatenate(halves(right), axis=right_dim), left_dim, right_dim)


def dot_wide_left(left, right):
    both = dot(jnp.concatenate(halves(left), axis=1), right, 0, 0)
    width = left.shape[1]
    return both[:width] + both[width:]


def rows_of(shape):
    return lax.broadcasted_iota(jnp.int32, shape, 0).astype(F32)


def decay_weights(rate):
    shape = (BLOCK, BLOCK)
    spacing = rows_of(shape) - lax.broadcasted_iota(jnp.int32, shape, 1).astype(F32)
    return jnp.where(spacing >= 0, jnp.exp(-rate * jnp.maximum(spacing, 0.0)), 0.0)


def block_rows(block):
    return slice(block * BLOCK, (block + 1) * BLOCK)


@dataclasses.dataclass
class Streamed:
    array: object


@dataclasses.dataclass
class Far:
    array: object


def cols_of(head):
    return slice(head * 128, (head + 1) * 128)


def start_copies(pairs, flags):
    copies = []
    for source, target in pairs:
        copy = pltpu.make_async_copy(source, target, flags.at[len(copies)])
        copy.start()
        copies.append(copy)
    return copies


def wait_all(copies):
    for copy in copies:
        copy.wait()


def memory_kernel(
    rates, far_keys, far_values, far_end, first, keys, values, end, ready, done
):
    stores = []
    loads = []
    for block in range(2):
        rows = block_rows(block)
        pairs = ((far_keys, keys), (far_values, values))
        loads.append(
            start_copies([(f.at[rows, :], n.at[rows, :]) for f, n in pairs], ready.at[block])
        )
    to_last = BLOCK - 1.0 - rows_of((BLOCK, 128))
    for block in range(2):
        rows = block_rows(block)
        wait_all(loads[block])
        for head in range(4):
            cols = cols_of(head)
            wide = keys[rows, cols].astype(F32) * jnp.exp(-rates[head] * to_last)
            update = dot_wide_left(wide, values[rows, cols])
            if block == 0:
                first[head] = update
            else:
                full = jnp.exp(jnp.full((128, 128), -BLOCK * rates[head], F32))
                end[head] = full * first[head] + update
                store = pltpu.make_async_copy(end.at[head], far_end.at[head], done.at[head])
                store.start()
                stores.append(store)
    wait_all(stores)


def rate_row(table, head):
    return table[1 + head : 2 + head, 0:128]


def inside_kernel(rates, queries, keys, values, gain, probs, inside, table):
    table[0:1, :] = gain[...]
    for head in range(4):
        table[1 + head : 2 + head, :] = jnp.full((1, table.shape[1]), rates[head], F32)
    for head in range(4):
        cols = cols_of(head)
        weights = decay_weights(rates[head])
        for block in range(2):
            rows = block_rows(block)
            scores = dot(queries[rows, cols], keys[rows, cols], 1, 1)
            low = (scores * weights).astype(BF16)
            probs[head, block] = low
            inside[rows, cols] = dot(low, values[rows, cols], 1, 0)


def carried_kernel(
    table, queries, entering, first, far_inside, out_grad, attention, sums, inside, ready
):
    loads = []
    for block in range(2):
        rows = block_rows(block)
        load = pltpu.make_async_copy(
            far_inside.at[rows, :], inside.at[rows, :], ready.at[block]
        )
        load.start()
        loads.append(load)
    after_start = rows_of((BLOCK, 128)) + 1.0
    squares, products = [], []
    for block in range(2):
        rows = block_rows(block)
        for head in range(4):
            cols = cols_of(head)
            memory = entering[head]
            if block == 1:
                memory = jnp.exp(-BLOCK * rate_row(table, head)) * memory + first[head]
            leading = jnp.exp(-rate_row(table, head) * after_start)
            carried = dot_wide_right(queries[rows, cols], memory, 1, 0)
            attention[rows, cols] = carried * leading
        loads[block].wait()
        square = product = None
        for head in range(4):
            cols = cols_of(head)
            out = inside[rows, cols] + attention[rows, cols]
            attention[rows, cols] = out
            grad = out_grad[rows, cols].astype(F32) * table[0:1, cols]
            square = out * out if square is None else square + out * out
            product = grad * out if product is None else product + grad * out
        for part, flat in ((square, squares), (product, products)):
            for tile in range(2):
                turned = part[tile * 128 : (tile + 1) * 128, :].T
                flat.append(jnp.sum(turned, axis=0, keepdims=True))
    both = jnp.concatenate(squares + products, axis=0)
    for peer in range(sums.shape[0]):
        sums[peer] = both


def per_token(row):
    return jnp.broadcast_to(row, (128, 128)).T


def scales_of(features, sums, block):
    total = sums[0]
    for peer in range(1, sums.shape[0]):
        total = total + sums[peer]
    scale = lax.rsqrt(total[0:4] / features + EPSILON)
    coeff = scale * total[4:8] / features
    tiles = (2 * block, 2 * block + 1)
    return tuple(
        jnp.concatenate([per_token(part[tile : tile + 1]) for tile in tiles], axis=0)
        for part in (scale, coeff)
    )


def attention_grad(attention, out_grad, gain, scale, coeff):
    normed = attention * scale
    grad = out_grad.astype(F32) * gain
    return normed, (scale * (grad - normed * coeff)).astype(BF16)


def grad_kernel(
    features, table, sums, queries, attention, out_grad, far_end, end, done
):
    stores = []
    from_start = rows_of((BLOCK, 128))
    for block in (1, 0):
        rows = block_rows(block)
        scale, coeff = scales_of(features, sums, block)
        for head in range(4):
            cols = cols_of(head)
            _, low = attention_grad(
                attention[rows, cols], out_grad[rows, cols], table[0:1, cols], scale, coeff
            )
            start = jnp.exp(-rate_row(table, head) * from_start)
            gathered = dot_wide_left(queries[rows, cols].astype(F32) * start, low)
            if block == 1:
                end[head] = gathered
            else:
                end[head] = jnp.exp(-BLOCK * rate_row(table, head)) * end[head] + gathered
                store = pltpu.make_async_copy(end.at[head], far_end.at[head], done.at[head])
                store.start()
                stores.append(store)
    wait_all(stores)


def local_kernel(
    features,
    rates,
    queries,
    keys,
    values,
    out_grad,
    probs,
    entering,
    first,
    sums,
    attention,
    gain,
    query_grad,
    normed_out,
    key_part,
    value_part,
    second,
):
    after_start = rows_of((BLOCK, 128)) + 1.0
    for block in range(2):
        rows = block_rows(block)
        scale, coeff = scales_of(features, sums, block)
        for head in range(4):
            cols = cols_of(head)
            weights = decay_weights(rates[head])
            memory = entering[head]
            if block == 1:
                full = jnp.exp(jnp.full((128, 128), -BLOCK * rates[head], F32))
                memory = full * memory + first[head]
            leading = jnp.exp(-rates[head] * after_start)
            normed, grad = attention_grad(
                attention[rows, cols], out_grad[rows, cols], gain[:, cols], scale, coeff
            )
            normed_out[rows, cols] = (normed * gain[:, cols]).astype(BF16)
            low = (dot(grad, values[rows, cols], 1, 1) * weights).astype(BF16)
            carried = dot_wide_right(grad, memory, 1, 1) * leading
            query_grad[rows, cols] = (dot(low, keys[rows, cols], 1, 0) + carried).astype(BF16)
            key_part[rows, cols] = dot(low, queries[rows, cols], 0, 0)
            value_part[rows, cols] = dot(probs[head, block], grad, 0, 0)
            if block == 1:
                start = jnp.exp(-rates[head] * (after_start - 1.0))
                second[head] = dot_wide_left(queries[rows, cols].astype(F32) * start, grad)


def finish_kernel(
    rates,
    keys,
    values,
    far_key_part,
    far_value_part,
    after,
    second,
    far_key_grad,
    far_value_grad,
    key_part,
    value_part,
    key_more,
    value_more,
    key_grad,
    value_grad,
    ready,
    done,
):
    loads, stores = [], []
    for block in range(2):
        rows = block_rows(block)
        pairs = ((far_key_part, key_part), (far_value_part, value_part))
        loads.append(
            start_copies([(f.at[rows, :], n.at[rows, :]) for f, n in pairs], ready.at[block])
        )
    to_end = BLOCK - rows_of((BLOCK, 128))
    for block in range(2):
        rows = block_rows(block)
        for head in range(4):
            cols = cols_of(head)
            ending = jnp.exp(-rates[head] * to_end)
            backlog = after[head]
            if block == 0:
                full = jnp.exp(jnp.full((128, 128), -BLOCK * rates[head], F32))
                backlog = full * backlog + second[head]
            key_more[:, cols] = dot_wide_right(values[rows, cols], backlog, 1, 1) * ending
            value_more[:, cols] = dot_wide_right(keys[rows, cols], backlog, 1, 0) * ending
        wait_all(loads[block])
        for half in range(4):
            span = slice(block * BLOCK + half * 64, block * BLOCK + half * 64 + 64)
            own = slice(half * 64, half * 64 + 64)
            key_grad[span, :] = (key_part[span, :] + key_more[own, :]).astype(BF16)
            value_grad[span, :] = (value_part[span, :] + value_more[own, :]).astype(BF16)
            pairs = ((key_grad, far_key_grad), (value_grad, far_value_grad))
            stores += start_copies(
                [(n.at[span, :], f.at[span, :]) for n, f in pairs], done.at[4 * block + half]
            )
    wait_all(stores)


def shape(*dims, dtype=F32):
    return jax.ShapeDtypeStruct(dims, dtype)


def near(array):
    return pltpu.with_memory_space_constraint(array, pltpu.VMEM)


def place_of(item):
    if isinstance(item, Far):
        return pl.BlockSpec(memory_space=pltpu.HBM)
    return pl.BlockSpec() if isinstance(item, Streamed) else VMEM


def bare(item):
    return item.array if isinstance(item, (Far, Streamed)) else item


def call(kernel, name, outs, *operands, grant=GRANT, rates=None, scratch=()):
    small = [] if rates is None else [rates]
    return pl.pallas_call(
        kernel,
        in_specs=[SMEM] * len(small) + [place_of(item) for item in operands],
        out_specs=tuple(place_of(item) for item in outs),
        out_shape=tuple(bare(item) for item in outs),
        scratch_shapes=scratch,
        name=name,
        cost_estimate=pl.CostEstimate(
            flops=400_000_000, bytes_accessed=4_000_000, transcendentals=300_000
        ),
        compiler_params=pltpu.CompilerParams(vmem_limit_bytes=grant),
    )(*small, *map(bare, operands))


def scan_total(table, pieces, reverse, filled):
    count, rows, lanes = pieces.shape

    def kernel(table_ref, piece_ref, _, total_ref):
        order = range(count - 1, -1, -1) if reverse else range(count)
        running = None
        for k in order:
            piece = piece_ref[k]
            running = piece if running is None else running * table_ref[0] + piece
        for peer in range(total_ref.shape[0]):
            total_ref[peer] = running

    return pl.pallas_call(
        kernel,
        in_specs=[SMEM, VMEM, VMEM],
        out_specs=VMEM,
        out_shape=pltpu.VMEM((lax.axis_size(LINE[0]), rows, lanes), F32),
        name="scan_total",
        compiler_params=pltpu.CompilerParams(vmem_limit_bytes=GRANT),
    )(table, near(pieces), near(filled))


def scan_prefix(table, pieces, totals, reverse):
    count, rows, lanes = pieces.shape
    first = 5 if reverse else 1

    def kernel(table_ref, piece_ref, total_ref, prefix_ref):
        order = list(range(count - 1, -1, -1) if reverse else range(count))
        running = total_ref[0] * table_ref[first]
        for peer in range(1, total_ref.shape[0]):
            running = running + total_ref[peer] * table_ref[first + peer]
        for k in order:
            prefix_ref[k] = running
            if k != order[-1]:
                running = running * table_ref[0] + piece_ref[k]

    return pl.pallas_call(
        kernel,
        in_specs=[SMEM, VMEM, VMEM],
        out_specs=VMEM,
        out_shape=pltpu.VMEM((count, rows, lanes), F32),
        name="scan_prefix",
        compiler_params=pltpu.CompilerParams(vmem_limit_bytes=GRANT),
    )(table, near(pieces), near(totals))


def line_table(decay_rates, token_count):
    far, near = lax.axis_index(LINE[0]), lax.axis_index(LINE[1])
    far_size, near_size = lax.axis_size(LINE[0]), lax.axis_size(LINE[1])
    rate = lax.dynamic_index_in_dim(
        decay_rates, near * decay_rates.shape[0] // near_size, 0, keepdims=False
    )
    slot = jnp.arange(1 + 2 * far_size)
    earlier = far - slot
    later = slot - 1 - far_size - far - 1
    steps = jnp.where(slot > far_size, later, earlier) * near_size
    steps = jnp.where(slot == 0, 1, steps)
    weights = jnp.exp(-rate * token_count * jnp.maximum(steps, 0).astype(F32))
    return jnp.where(steps >= 0, weights, 0.0)


def along_context(table, state, reverse, filled):
    near_size, far_size = lax.axis_size(LINE[1]), lax.axis_size(LINE[0])
    lanes = state.shape[-1]
    pieces = lax.all_to_all(state.reshape(near_size, -1, lanes), LINE[1], 0, 0)
    totals = lax.all_to_all(scan_total(table, pieces, reverse, filled), LINE[0], 0, 0)
    prefix = scan_prefix(table, pieces, totals, reverse)
    return lax.all_to_all(prefix, LINE[1], 0, 0).reshape(state.shape)


def on_device(queries, key_rows, value_rows, decay_rates, norm_gain, out_grad):
    tokens, width = queries.shape
    heads = decay_rates.shape[0]
    features = float(width * lax.axis_size(SIDE))
    gain = norm_gain[None, :]
    table = line_table(decay_rates, tokens)
    state = shape(heads, 128, 128)
    wide, narrow = shape(tokens, width), shape(tokens, width, dtype=BF16)
    tables = shape(heads, 2, BLOCK, BLOCK, dtype=BF16)
    state_near, wide_near = pltpu.VMEM(state.shape, F32), pltpu.VMEM(wide.shape, F32)
    far_q, far_k, far_v, far_grad = map(Streamed, (queries, key_rows, value_rows, out_grad))
    narrow_near, flags = pltpu.VMEM(narrow.shape, BF16), pltpu.SemaphoreType.DMA((2, 2))
    memory_end, memory_first = call(
        memory_kernel,
        "memory",
        (Far(state), state_near),
        Far(key_rows),
        Far(value_rows),
        grant=None,
        rates=decay_rates,
        scratch=(narrow_near, narrow_near, state_near, flags, pltpu.SemaphoreType.DMA((4,))),
    )
    probs, inside, aux = call(
        inside_kernel,
        "inside",
        (Streamed(tables), Streamed(wide), pltpu.VMEM((8, width), F32)),
        far_q,
        far_k,
        far_v,
        Streamed(gain),
        grant=None,
        rates=decay_rates,
    )
    entering = along_context(table, memory_end, False, aux)
    attention, sums = call(
        carried_kernel,
        "carried",
        (wide_near, pltpu.VMEM((lax.axis_size(SIDE), 8, 128), F32)),
        near(aux),
        near(queries),
        near(entering),
        near(memory_first),
        Far(inside),
        near(out_grad),
        grant=None,
        scratch=(wide_near, pltpu.SemaphoreType.DMA((2,))),
    )
    sums = lax.all_to_all(sums, SIDE, 0, 0)
    (backlog_end,) = call(
        functools.partial(grad_kernel, features),
        "grad",
        (Far(state),),
        near(aux),
        near(sums),
        near(queries),
        near(attention),
        near(out_grad),
        grant=None,
        scratch=(state_near, pltpu.SemaphoreType.DMA((4,))),
    )
    query_grad, normed_out, key_part, value_part, backlog_second = call(
        functools.partial(local_kernel, features),
        "local",
        (Streamed(narrow), Streamed(narrow), Streamed(wide), Streamed(wide), state_near),
        far_q,
        far_k,
        far_v,
        far_grad,
        Streamed(probs),
        near(entering),
        near(memory_first),
        near(sums),
        near(attention),
        Streamed(gain),
        grant=None,
        rates=decay_rates,
    )
    after = along_context(table, backlog_end, True, backlog_second)
    more = pltpu.VMEM((BLOCK, width), F32)
    key_grad, value_grad = call(
        finish_kernel,
        "finish",
        (Far(narrow), Far(narrow)),
        near(key_rows),
        near(value_rows),
        Far(key_part),
        Far(value_part),
        near(after),
        near(backlog_second),
        grant=None,
        rates=decay_rates,
        scratch=(wide_near, wide_near, more, more, narrow_near, narrow_near, flags, pltpu.SemaphoreType.DMA((8, 2))),
    )
    return (normed_out, query_grad, key_grad, value_grad)


def solution(mesh):
    split = Mesh(mesh.devices.reshape(4, 16, 4, 2), LINE + SIDE)
    rows = P(LINE, SIDE)
    return jax.shard_map(
        on_device,
        mesh=split,
        in_specs=(rows, rows, rows, P(SIDE), P(SIDE), rows),
        out_specs=(rows, rows, rows, rows),
        check_vma=False,
    )
```

```python
import dataclasses
import functools

import jax
import jax.numpy as jnp
from jax import lax
from jax.experimental import pallas as pl
from jax.experimental.pallas import tpu as pltpu
from jax.sharding import Mesh
from jax.sharding import PartitionSpec as P

BLOCK = 256
LINE = ("ctx_0", "ctx_1")
SIDE = ("row", "core")
EPSILON = 1e-06
GRANT = 12 << 20
F32 = jnp.float32
BF16 = jnp.bfloat16
SMEM = pl.BlockSpec(memory_space=pltpu.SMEM)
VMEM = pl.BlockSpec(memory_space=pltpu.VMEM)


def dot(left, right, left_dim, right_dim):
    return lax.dot_general(
        left, right, (((left_dim,), (right_dim,)), ((), ())), preferred_element_type=F32
    )


def halves(wide):
    high = wide.astype(BF16)
    return high, (wide - high.astype(F32)).astype(BF16)


def dot_wide_right(left, right, left_dim, right_dim):
    twice = jnp.concatenate([left, left], axis=left_dim)
    return dot(twice, jnp.concatenate(halves(right), axis=right_dim), left_dim, right_dim)


def dot_wide_left(left, right):
    both = dot(jnp.concatenate(halves(left), axis=1), right, 0, 0)
    width = left.shape[1]
    return both[:width] + both[width:]


def rows_of(shape):
    return lax.broadcasted_iota(jnp.int32, shape, 0).astype(F32)


def decay_weights(rate):
    shape = (BLOCK, BLOCK)
    spacing = rows_of(shape) - lax.broadcasted_iota(jnp.int32, shape, 1).astype(F32)
    return jnp.where(spacing >= 0, jnp.exp(-rate * jnp.maximum(spacing, 0.0)), 0.0)


def block_rows(block):
    return slice(block * BLOCK, (block + 1) * BLOCK)


@dataclasses.dataclass
class Streamed:
    array: object


@dataclasses.dataclass
class Far:
    array: object


def cols_of(head):
    return slice(head * 128, (head + 1) * 128)


def start_copies(pairs, flags):
    copies = []
    for source, target in pairs:
        copy = pltpu.make_async_copy(source, target, flags.at[len(copies)])
        copy.start()
        copies.append(copy)
    return copies


def wait_all(copies):
    for copy in copies:
        copy.wait()


def memory_kernel(
    rates, far_keys, far_values, far_end, first, keys, values, end, ready, done
):
    stores = []
    loads = []
    for block in range(2):
        rows = block_rows(block)
        pairs = ((far_keys, keys), (far_values, values))
        loads.append(
            start_copies([(f.at[rows, :], n.at[rows, :]) for f, n in pairs], ready.at[block])
        )
    to_last = BLOCK - 1.0 - rows_of((BLOCK, 128))
    for block in range(2):
        rows = block_rows(block)
        wait_all(loads[block])
        for head in range(4):
            cols = cols_of(head)
            wide = keys[rows, cols].astype(F32) * jnp.exp(-rates[head] * to_last)
            update = dot_wide_left(wide, values[rows, cols])
            if block == 0:
                first[head] = update
            else:
                full = jnp.exp(jnp.full((128, 128), -BLOCK * rates[head], F32))
                end[head] = full * first[head] + update
                store = pltpu.make_async_copy(end.at[head], far_end.at[head], done.at[head])
                store.start()
                stores.append(store)
    wait_all(stores)


def rate_row(table, head):
    return table[1 + head : 2 + head, 0:128]


def inside_kernel(rates, queries, keys, values, gain, probs, inside, table):
    table[0:1, :] = gain[...]
    for head in range(4):
        table[1 + head : 2 + head, :] = jnp.full((1, table.shape[1]), rates[head], F32)
    for head in range(4):
        cols = cols_of(head)
        weights = decay_weights(rates[head])
        for block in range(2):
            rows = block_rows(block)
            scores = dot(queries[rows, cols], keys[rows, cols], 1, 1)
            low = (scores * weights).astype(BF16)
            probs[head, block] = low
            inside[rows, cols] = dot(low, values[rows, cols], 1, 0)


def carried_kernel(
    table, queries, entering, first, far_inside, out_grad, attention, sums, inside, ready
):
    loads = []
    for block in range(2):
        rows = block_rows(block)
        load = pltpu.make_async_copy(
            far_inside.at[rows, :], inside.at[rows, :], ready.at[block]
        )
        load.start()
        loads.append(load)
    after_start = rows_of((BLOCK, 128)) + 1.0
    squares, products = [], []
    for block in range(2):
        rows = block_rows(block)
        for head in range(4):
            cols = cols_of(head)
            memory = entering[head]
            if block == 1:
                memory = jnp.exp(-BLOCK * rate_row(table, head)) * memory + first[head]
            leading = jnp.exp(-rate_row(table, head) * after_start)
            carried = dot_wide_right(queries[rows, cols], memory, 1, 0)
            attention[rows, cols] = carried * leading
        loads[block].wait()
        square = product = None
        for head in range(4):
            cols = cols_of(head)
            out = inside[rows, cols] + attention[rows, cols]
            attention[rows, cols] = out
            grad = out_grad[rows, cols].astype(F32) * table[0:1, cols]
            square = out * out if square is None else square + out * out
            product = grad * out if product is None else product + grad * out
        for part, flat in ((square, squares), (product, products)):
            for tile in range(2):
                turned = part[tile * 128 : (tile + 1) * 128, :].T
                flat.append(jnp.sum(turned, axis=0, keepdims=True))
    both = jnp.concatenate(squares + products, axis=0)
    for peer in range(sums.shape[0]):
        sums[peer] = both


def per_token(row):
    return jnp.broadcast_to(row, (128, 128)).T


def scales_of(features, sums, block):
    total = sums[0]
    for peer in range(1, sums.shape[0]):
        total = total + sums[peer]
    scale = lax.rsqrt(total[0:4] / features + EPSILON)
    coeff = scale * total[4:8] / features
    tiles = (2 * block, 2 * block + 1)
    return tuple(
        jnp.concatenate([per_token(part[tile : tile + 1]) for tile in tiles], axis=0)
        for part in (scale, coeff)
    )


def attention_grad(attention, out_grad, gain, scale, coeff):
    normed = attention * scale
    grad = out_grad.astype(F32) * gain
    return normed, (scale * (grad - normed * coeff)).astype(BF16)


def grad_kernel(
    features, table, sums, queries, attention, out_grad, far_end, end, done
):
    stores = []
    from_start = rows_of((BLOCK, 128))
    for block in (1, 0):
        rows = block_rows(block)
        scale, coeff = scales_of(features, sums, block)
        for head in range(4):
            cols = cols_of(head)
            _, low = attention_grad(
                attention[rows, cols], out_grad[rows, cols], table[0:1, cols], scale, coeff
            )
            start = jnp.exp(-rate_row(table, head) * from_start)
            gathered = dot_wide_left(queries[rows, cols].astype(F32) * start, low)
            if block == 1:
                end[head] = gathered
            else:
                end[head] = jnp.exp(-BLOCK * rate_row(table, head)) * end[head] + gathered
                store = pltpu.make_async_copy(end.at[head], far_end.at[head], done.at[head])
                store.start()
                stores.append(store)
    wait_all(stores)


def local_kernel(
    features,
    rates,
    queries,
    keys,
    values,
    out_grad,
    probs,
    entering,
    first,
    sums,
    attention,
    gain,
    query_grad,
    normed_out,
    key_part,
    value_part,
    second,
):
    after_start = rows_of((BLOCK, 128)) + 1.0
    for block in range(2):
        rows = block_rows(block)
        scale, coeff = scales_of(features, sums, block)
        for head in range(4):
            cols = cols_of(head)
            weights = decay_weights(rates[head])
            memory = entering[head]
            if block == 1:
                full = jnp.exp(jnp.full((128, 128), -BLOCK * rates[head], F32))
                memory = full * memory + first[head]
            leading = jnp.exp(-rates[head] * after_start)
            normed, grad = attention_grad(
                attention[rows, cols], out_grad[rows, cols], gain[:, cols], scale, coeff
            )
            normed_out[rows, cols] = (normed * gain[:, cols]).astype(BF16)
            low = (dot(grad, values[rows, cols], 1, 1) * weights).astype(BF16)
            carried = dot_wide_right(grad, memory, 1, 1) * leading
            query_grad[rows, cols] = (dot(low, keys[rows, cols], 1, 0) + carried).astype(BF16)
            key_part[rows, cols] = dot(low, queries[rows, cols], 0, 0)
            value_part[rows, cols] = dot(probs[head, block], grad, 0, 0)
            if block == 1:
                start = jnp.exp(-rates[head] * (after_start - 1.0))
                second[head] = dot_wide_left(queries[rows, cols].astype(F32) * start, grad)


def settle_kernel(key_part, value_part, second, settled):
    settled[...] = key_part[0:8, 0:128] + value_part[0:8, 0:128] + second[0, 0:8, :]


def finish_kernel(
    table,
    keys,
    values,
    key_part,
    value_part,
    after,
    second,
    far_key_grad,
    far_value_grad,
    key_grad,
    value_grad,
    done,
):
    stores = []
    to_end = BLOCK - rows_of((BLOCK, 128))
    for block in range(2):
        rows = block_rows(block)
        for head in range(4):
            cols = cols_of(head)
            ending = jnp.exp(-rate_row(table, head) * to_end)
            backlog = after[head]
            if block == 0:
                full = jnp.exp(-BLOCK * rate_row(table, head))
                backlog = full * backlog + second[head]
            key_more = dot_wide_right(values[rows, cols], backlog, 1, 1) * ending
            value_more = dot_wide_right(keys[rows, cols], backlog, 1, 0) * ending
            key_grad[rows, cols] = (key_part[rows, cols] + key_more).astype(BF16)
            value_grad[rows, cols] = (value_part[rows, cols] + value_more).astype(BF16)
            pairs = ((key_grad, far_key_grad), (value_grad, far_value_grad))
            stores += start_copies(
                [(n.at[rows, cols], f.at[rows, cols]) for n, f in pairs],
                done.at[4 * block + head],
            )
    wait_all(stores)


def shape(*dims, dtype=F32):
    return jax.ShapeDtypeStruct(dims, dtype)


def near(array):
    return pltpu.with_memory_space_constraint(array, pltpu.VMEM)


def place_of(item):
    if isinstance(item, Far):
        return pl.BlockSpec(memory_space=pltpu.HBM)
    return pl.BlockSpec() if isinstance(item, Streamed) else VMEM


def bare(item):
    return item.array if isinstance(item, (Far, Streamed)) else item


def call(kernel, name, outs, *operands, grant=GRANT, rates=None, scratch=()):
    small = [] if rates is None else [rates]
    return pl.pallas_call(
        kernel,
        in_specs=[SMEM] * len(small) + [place_of(item) for item in operands],
        out_specs=tuple(place_of(item) for item in outs),
        out_shape=tuple(bare(item) for item in outs),
        scratch_shapes=scratch,
        name=name,
        cost_estimate=pl.CostEstimate(
            flops=400_000_000, bytes_accessed=4_000_000, transcendentals=300_000
        ),
        compiler_params=pltpu.CompilerParams(vmem_limit_bytes=grant),
    )(*small, *map(bare, operands))


def scan_total(table, pieces, reverse, filled):
    count, rows, lanes = pieces.shape

    def kernel(table_ref, piece_ref, _, total_ref):
        order = range(count - 1, -1, -1) if reverse else range(count)
        running = None
        for k in order:
            piece = piece_ref[k]
            running = piece if running is None else running * table_ref[0] + piece
        for peer in range(total_ref.shape[0]):
            total_ref[peer] = running

    return pl.pallas_call(
        kernel,
        in_specs=[SMEM, VMEM, VMEM],
        out_specs=VMEM,
        out_shape=pltpu.VMEM((lax.axis_size(LINE[0]), rows, lanes), F32),
        name="scan_total",
        compiler_params=pltpu.CompilerParams(vmem_limit_bytes=GRANT),
    )(table, near(pieces), near(filled))


def scan_prefix(table, pieces, totals, reverse):
    count, rows, lanes = pieces.shape
    first = 5 if reverse else 1

    def kernel(table_ref, piece_ref, total_ref, prefix_ref):
        order = list(range(count - 1, -1, -1) if reverse else range(count))
        running = total_ref[0] * table_ref[first]
        for peer in range(1, total_ref.shape[0]):
            running = running + total_ref[peer] * table_ref[first + peer]
        for k in order:
            prefix_ref[k] = running
            if k != order[-1]:
                running = running * table_ref[0] + piece_ref[k]

    return pl.pallas_call(
        kernel,
        in_specs=[SMEM, VMEM, VMEM],
        out_specs=VMEM,
        out_shape=pltpu.VMEM((count, rows, lanes), F32),
        name="scan_prefix",
        compiler_params=pltpu.CompilerParams(vmem_limit_bytes=GRANT),
    )(table, near(pieces), near(totals))


def line_table(decay_rates, token_count):
    far, near = lax.axis_index(LINE[0]), lax.axis_index(LINE[1])
    far_size, near_size = lax.axis_size(LINE[0]), lax.axis_size(LINE[1])
    rate = lax.dynamic_index_in_dim(
        decay_rates, near * decay_rates.shape[0] // near_size, 0, keepdims=False
    )
    slot = jnp.arange(1 + 2 * far_size)
    earlier = far - slot
    later = slot - 1 - far_size - far - 1
    steps = jnp.where(slot > far_size, later, earlier) * near_size
    steps = jnp.where(slot == 0, 1, steps)
    weights = jnp.exp(-rate * token_count * jnp.maximum(steps, 0).astype(F32))
    return jnp.where(steps >= 0, weights, 0.0)


def along_context(table, state, reverse, filled):
    near_size, far_size = lax.axis_size(LINE[1]), lax.axis_size(LINE[0])
    lanes = state.shape[-1]
    pieces = lax.all_to_all(state.reshape(near_size, -1, lanes), LINE[1], 0, 0)
    totals = lax.all_to_all(scan_total(table, pieces, reverse, filled), LINE[0], 0, 0)
    prefix = scan_prefix(table, pieces, totals, reverse)
    return lax.all_to_all(prefix, LINE[1], 0, 0).reshape(state.shape)


def on_device(queries, key_rows, value_rows, decay_rates, norm_gain, out_grad):
    tokens, width = queries.shape
    heads = decay_rates.shape[0]
    features = float(width * lax.axis_size(SIDE))
    gain = norm_gain[None, :]
    table = line_table(decay_rates, tokens)
    state = shape(heads, 128, 128)
    wide, narrow = shape(tokens, width), shape(tokens, width, dtype=BF16)
    tables = shape(heads, 2, BLOCK, BLOCK, dtype=BF16)
    state_near, wide_near = pltpu.VMEM(state.shape, F32), pltpu.VMEM(wide.shape, F32)
    far_q, far_k, far_v, far_grad = map(Streamed, (queries, key_rows, value_rows, out_grad))
    narrow_near, flags = pltpu.VMEM(narrow.shape, BF16), pltpu.SemaphoreType.DMA((2, 2))
    memory_end, memory_first = call(
        memory_kernel,
        "memory",
        (Far(state), state_near),
        Far(key_rows),
        Far(value_rows),
        grant=None,
        rates=decay_rates,
        scratch=(narrow_near, narrow_near, state_near, flags, pltpu.SemaphoreType.DMA((4,))),
    )
    probs, inside, aux = call(
        inside_kernel,
        "inside",
        (Streamed(tables), Streamed(wide), pltpu.VMEM((8, width), F32)),
        far_q,
        far_k,
        far_v,
        Streamed(gain),
        grant=None,
        rates=decay_rates,
    )
    entering = along_context(table, memory_end, False, aux)
    attention, sums = call(
        carried_kernel,
        "carried",
        (wide_near, pltpu.VMEM((lax.axis_size(SIDE), 8, 128), F32)),
        near(aux),
        near(queries),
        near(entering),
        near(memory_first),
        Far(inside),
        near(out_grad),
        grant=None,
        scratch=(wide_near, pltpu.SemaphoreType.DMA((2,))),
    )
    sums = lax.all_to_all(sums, SIDE, 0, 0)
    (backlog_end,) = call(
        functools.partial(grad_kernel, features),
        "grad",
        (Far(state),),
        near(aux),
        near(sums),
        near(queries),
        near(attention),
        near(out_grad),
        grant=None,
        scratch=(state_near, pltpu.SemaphoreType.DMA((4,))),
    )
    query_grad, normed_out, key_part, value_part, backlog_second = call(
        functools.partial(local_kernel, features),
        "local",
        (Streamed(narrow), Streamed(narrow), Streamed(wide), Streamed(wide), state_near),
        far_q,
        far_k,
        far_v,
        far_grad,
        Streamed(probs),
        near(entering),
        near(memory_first),
        near(sums),
        near(attention),
        Streamed(gain),
        grant=None,
        rates=decay_rates,
    )
    (settled,) = call(
        settle_kernel,
        "settle",
        (pltpu.VMEM((8, 128), F32),),
        near(key_part),
        near(value_part),
        near(backlog_second),
    )
    after = along_context(table, backlog_end, True, settled)
    key_grad, value_grad = call(
        finish_kernel,
        "finish",
        (Far(narrow), Far(narrow)),
        near(aux),
        near(key_rows),
        near(value_rows),
        near(key_part),
        near(value_part),
        near(after),
        near(backlog_second),
        scratch=(narrow_near, narrow_near, pltpu.SemaphoreType.DMA((8, 2))),
    )
    return (normed_out, query_grad, key_grad, value_grad)


def solution(mesh):
    split = Mesh(mesh.devices.reshape(4, 16, 4, 2), LINE + SIDE)
    rows = P(LINE, SIDE)
    return jax.shard_map(
        on_device,
        mesh=split,
        in_specs=(rows, rows, rows, P(SIDE), P(SIDE), rows),
        out_specs=(rows, rows, rows, rows),
        check_vma=False,
    )
```

```python
import dataclasses
import functools

import jax
import jax.numpy as jnp
from jax import lax
from jax.experimental import pallas as pl
from jax.experimental.pallas import tpu as pltpu
from jax.sharding import Mesh
from jax.sharding import PartitionSpec as P

BLOCK = 256
LINE = ("ctx_0", "ctx_1")
SIDE = ("row", "core")
EPSILON = 1e-06
GRANT = 12 << 20
F32 = jnp.float32
BF16 = jnp.bfloat16
SMEM = pl.BlockSpec(memory_space=pltpu.SMEM)
VMEM = pl.BlockSpec(memory_space=pltpu.VMEM)


def dot(left, right, left_dim, right_dim):
    return lax.dot_general(
        left, right, (((left_dim,), (right_dim,)), ((), ())), preferred_element_type=F32
    )


def halves(wide):
    high = wide.astype(BF16)
    return high, (wide - high.astype(F32)).astype(BF16)


def dot_wide_right(left, right, left_dim, right_dim):
    twice = jnp.concatenate([left, left], axis=left_dim)
    return dot(twice, jnp.concatenate(halves(right), axis=right_dim), left_dim, right_dim)


def dot_wide_left(left, right):
    both = dot(jnp.concatenate(halves(left), axis=1), right, 0, 0)
    width = left.shape[1]
    return both[:width] + both[width:]


def rows_of(shape):
    return lax.broadcasted_iota(jnp.int32, shape, 0).astype(F32)


def decay_weights(rate):
    shape = (BLOCK, BLOCK)
    spacing = rows_of(shape) - lax.broadcasted_iota(jnp.int32, shape, 1).astype(F32)
    return jnp.where(spacing >= 0, jnp.exp(-rate * jnp.maximum(spacing, 0.0)), 0.0)


def block_rows(block):
    return slice(block * BLOCK, (block + 1) * BLOCK)


@dataclasses.dataclass
class Streamed:
    array: object


@dataclasses.dataclass
class Far:
    array: object


def cols_of(head):
    return slice(head * 128, (head + 1) * 128)


def start_copies(pairs, flags):
    copies = []
    for source, target in pairs:
        copy = pltpu.make_async_copy(source, target, flags.at[len(copies)])
        copy.start()
        copies.append(copy)
    return copies


def wait_all(copies):
    for copy in copies:
        copy.wait()


def memory_kernel(
    rates, far_keys, far_values, far_end, first, keys, values, end, ready, done
):
    stores = []
    loads = []
    for block in range(2):
        rows = block_rows(block)
        pairs = ((far_keys, keys), (far_values, values))
        loads.append(
            start_copies([(f.at[rows, :], n.at[rows, :]) for f, n in pairs], ready.at[block])
        )
    to_last = BLOCK - 1.0 - rows_of((BLOCK, 128))
    for block in range(2):
        rows = block_rows(block)
        wait_all(loads[block])
        for head in range(4):
            cols = cols_of(head)
            wide = keys[rows, cols].astype(F32) * jnp.exp(-rates[head] * to_last)
            update = dot_wide_left(wide, values[rows, cols])
            if block == 0:
                first[head] = update
            else:
                full = jnp.exp(jnp.full((128, 128), -BLOCK * rates[head], F32))
                end[head] = full * first[head] + update
                store = pltpu.make_async_copy(end.at[head], far_end.at[head], done.at[head])
                store.start()
                stores.append(store)
    wait_all(stores)


def rate_row(table, head):
    return table[1 + head : 2 + head, 0:128]


def inside_kernel(rates, queries, keys, values, gain, probs, inside, table):
    table[0:1, :] = gain[...]
    for head in range(4):
        table[1 + head : 2 + head, :] = jnp.full((1, table.shape[1]), rates[head], F32)
    for head in range(4):
        cols = cols_of(head)
        weights = decay_weights(rates[head])
        for block in range(2):
            rows = block_rows(block)
            scores = dot(queries[rows, cols], keys[rows, cols], 1, 1)
            low = (scores * weights).astype(BF16)
            probs[head, block] = low
            inside[rows, cols] = dot(low, values[rows, cols], 1, 0)


def carried_kernel(
    table, queries, entering, first, far_inside, out_grad, attention, sums, inside, ready
):
    loads = []
    for block in range(2):
        rows = block_rows(block)
        load = pltpu.make_async_copy(
            far_inside.at[rows, :], inside.at[rows, :], ready.at[block]
        )
        load.start()
        loads.append(load)
    after_start = rows_of((BLOCK, 128)) + 1.0
    squares, products = [], []
    for block in range(2):
        rows = block_rows(block)
        for head in range(4):
            cols = cols_of(head)
            memory = entering[head]
            if block == 1:
                memory = jnp.exp(-BLOCK * rate_row(table, head)) * memory + first[head]
            leading = jnp.exp(-rate_row(table, head) * after_start)
            carried = dot_wide_right(queries[rows, cols], memory, 1, 0)
            attention[rows, cols] = carried * leading
    for block in range(2):
        rows = block_rows(block)
        loads[block].wait()
        square = product = None
        for head in range(4):
            cols = cols_of(head)
            out = inside[rows, cols] + attention[rows, cols]
            attention[rows, cols] = out
            grad = out_grad[rows, cols].astype(F32) * table[0:1, cols]
            square = out * out if square is None else square + out * out
            product = grad * out if product is None else product + grad * out
        for part, flat in ((square, squares), (product, products)):
            for tile in range(2):
                turned = part[tile * 128 : (tile + 1) * 128, :].T
                flat.append(jnp.sum(turned, axis=0, keepdims=True))
    both = jnp.concatenate(squares + products, axis=0)
    for peer in range(sums.shape[0]):
        sums[peer] = both


def per_token(row):
    return jnp.broadcast_to(row, (128, 128)).T


def scales_of(features, sums, block):
    total = sums[0]
    for peer in range(1, sums.shape[0]):
        total = total + sums[peer]
    scale = lax.rsqrt(total[0:4] / features + EPSILON)
    coeff = scale * total[4:8] / features
    tiles = (2 * block, 2 * block + 1)
    return tuple(
        jnp.concatenate([per_token(part[tile : tile + 1]) for tile in tiles], axis=0)
        for part in (scale, coeff)
    )


def attention_grad(attention, out_grad, gain, scale, coeff):
    normed = attention * scale
    grad = out_grad.astype(F32) * gain
    return normed, (scale * (grad - normed * coeff)).astype(BF16)


def grad_kernel(
    features, table, sums, queries, attention, out_grad, far_end, end, done
):
    stores = []
    from_start = rows_of((BLOCK, 128))
    scales = [scales_of(features, sums, block) for block in range(2)]
    for head in range(4):
        cols = cols_of(head)
        start = jnp.exp(-rate_row(table, head) * from_start)
        gathered = []
        for block in range(2):
            rows = block_rows(block)
            scale, coeff = scales[block]
            _, low = attention_grad(
                attention[rows, cols], out_grad[rows, cols], table[0:1, cols], scale, coeff
            )
            gathered.append(dot_wide_left(queries[rows, cols].astype(F32) * start, low))
        end[head] = jnp.exp(-BLOCK * rate_row(table, head)) * gathered[1] + gathered[0]
        store = pltpu.make_async_copy(end.at[head], far_end.at[head], done.at[head])
        store.start()
        stores.append(store)
    wait_all(stores)


def local_kernel(
    features,
    rates,
    queries,
    keys,
    values,
    out_grad,
    probs,
    entering,
    first,
    sums,
    attention,
    gain,
    query_grad,
    normed_out,
    key_part,
    value_part,
    second,
):
    after_start = rows_of((BLOCK, 128)) + 1.0
    for block in range(2):
        rows = block_rows(block)
        scale, coeff = scales_of(features, sums, block)
        for head in range(4):
            cols = cols_of(head)
            weights = decay_weights(rates[head])
            memory = entering[head]
            if block == 1:
                full = jnp.exp(jnp.full((128, 128), -BLOCK * rates[head], F32))
                memory = full * memory + first[head]
            leading = jnp.exp(-rates[head] * after_start)
            normed, grad = attention_grad(
                attention[rows, cols], out_grad[rows, cols], gain[:, cols], scale, coeff
            )
            normed_out[rows, cols] = (normed * gain[:, cols]).astype(BF16)
            low = (dot(grad, values[rows, cols], 1, 1) * weights).astype(BF16)
            carried = dot_wide_right(grad, memory, 1, 1) * leading
            query_grad[rows, cols] = (dot(low, keys[rows, cols], 1, 0) + carried).astype(BF16)
            key_part[rows, cols] = dot(low, queries[rows, cols], 0, 0)
            value_part[rows, cols] = dot(probs[head, block], grad, 0, 0)
            if block == 1:
                start = jnp.exp(-rates[head] * (after_start - 1.0))
                second[head] = dot_wide_left(queries[rows, cols].astype(F32) * start, grad)


def settle_kernel(key_part, value_part, second, settled):
    settled[...] = key_part[0:8, 0:128] + value_part[0:8, 0:128] + second[0, 0:8, :]


def finish_kernel(
    table,
    keys,
    values,
    key_part,
    value_part,
    after,
    second,
    far_key_grad,
    far_value_grad,
    key_grad,
    value_grad,
    done,
):
    stores = []
    to_end = BLOCK - rows_of((BLOCK, 128))
    for block in range(2):
        rows = block_rows(block)
        for head in range(4):
            cols = cols_of(head)
            ending = jnp.exp(-rate_row(table, head) * to_end)
            backlog = after[head]
            if block == 0:
                full = jnp.exp(-BLOCK * rate_row(table, head))
                backlog = full * backlog + second[head]
            key_more = dot_wide_right(values[rows, cols], backlog, 1, 1) * ending
            value_more = dot_wide_right(keys[rows, cols], backlog, 1, 0) * ending
            key_grad[rows, cols] = (key_part[rows, cols] + key_more).astype(BF16)
            value_grad[rows, cols] = (value_part[rows, cols] + value_more).astype(BF16)
            pairs = ((key_grad, far_key_grad), (value_grad, far_value_grad))
            stores += start_copies(
                [(n.at[rows, cols], f.at[rows, cols]) for n, f in pairs],
                done.at[4 * block + head],
            )
    wait_all(stores)


def shape(*dims, dtype=F32):
    return jax.ShapeDtypeStruct(dims, dtype)


def near(array):
    return pltpu.with_memory_space_constraint(array, pltpu.VMEM)


def place_of(item):
    if isinstance(item, Far):
        return pl.BlockSpec(memory_space=pltpu.HBM)
    return pl.BlockSpec() if isinstance(item, Streamed) else VMEM


def bare(item):
    return item.array if isinstance(item, (Far, Streamed)) else item


def call(kernel, name, outs, *operands, grant=GRANT, rates=None, scratch=()):
    small = [] if rates is None else [rates]
    return pl.pallas_call(
        kernel,
        in_specs=[SMEM] * len(small) + [place_of(item) for item in operands],
        out_specs=tuple(place_of(item) for item in outs),
        out_shape=tuple(bare(item) for item in outs),
        scratch_shapes=scratch,
        name=name,
        cost_estimate=pl.CostEstimate(
            flops=400_000_000, bytes_accessed=4_000_000, transcendentals=300_000
        ),
        compiler_params=pltpu.CompilerParams(vmem_limit_bytes=grant),
    )(*small, *map(bare, operands))


def scan_total(table, pieces, reverse, filled):
    count, rows, lanes = pieces.shape

    def kernel(table_ref, piece_ref, _, total_ref):
        order = range(count - 1, -1, -1) if reverse else range(count)
        running = None
        for k in order:
            piece = piece_ref[k]
            running = piece if running is None else running * table_ref[0] + piece
        for peer in range(total_ref.shape[0]):
            total_ref[peer] = running

    return pl.pallas_call(
        kernel,
        in_specs=[SMEM, VMEM, VMEM],
        out_specs=VMEM,
        out_shape=pltpu.VMEM((lax.axis_size(LINE[0]), rows, lanes), F32),
        name="scan_total",
        compiler_params=pltpu.CompilerParams(vmem_limit_bytes=GRANT),
    )(table, near(pieces), near(filled))


def scan_prefix(table, pieces, totals, reverse):
    count, rows, lanes = pieces.shape
    first = 5 if reverse else 1

    def kernel(table_ref, piece_ref, total_ref, prefix_ref):
        order = list(range(count - 1, -1, -1) if reverse else range(count))
        running = total_ref[0] * table_ref[first]
        for peer in range(1, total_ref.shape[0]):
            running = running + total_ref[peer] * table_ref[first + peer]
        for k in order:
            prefix_ref[k] = running
            if k != order[-1]:
                running = running * table_ref[0] + piece_ref[k]

    return pl.pallas_call(
        kernel,
        in_specs=[SMEM, VMEM, VMEM],
        out_specs=VMEM,
        out_shape=pltpu.VMEM((count, rows, lanes), F32),
        name="scan_prefix",
        compiler_params=pltpu.CompilerParams(vmem_limit_bytes=GRANT),
    )(table, near(pieces), near(totals))


def line_table(decay_rates, token_count):
    far, near = lax.axis_index(LINE[0]), lax.axis_index(LINE[1])
    far_size, near_size = lax.axis_size(LINE[0]), lax.axis_size(LINE[1])
    rate = lax.dynamic_index_in_dim(
        decay_rates, near * decay_rates.shape[0] // near_size, 0, keepdims=False
    )
    slot = jnp.arange(1 + 2 * far_size)
    earlier = far - slot
    later = slot - 1 - far_size - far - 1
    steps = jnp.where(slot > far_size, later, earlier) * near_size
    steps = jnp.where(slot == 0, 1, steps)
    weights = jnp.exp(-rate * token_count * jnp.maximum(steps, 0).astype(F32))
    return jnp.where(steps >= 0, weights, 0.0)


def along_context(table, state, reverse, filled):
    near_size, far_size = lax.axis_size(LINE[1]), lax.axis_size(LINE[0])
    lanes = state.shape[-1]
    pieces = lax.all_to_all(state.reshape(near_size, -1, lanes), LINE[1], 0, 0)
    totals = lax.all_to_all(scan_total(table, pieces, reverse, filled), LINE[0], 0, 0)
    prefix = scan_prefix(table, pieces, totals, reverse)
    return lax.all_to_all(prefix, LINE[1], 0, 0).reshape(state.shape)


def on_device(queries, key_rows, value_rows, decay_rates, norm_gain, out_grad):
    tokens, width = queries.shape
    heads = decay_rates.shape[0]
    features = float(width * lax.axis_size(SIDE))
    gain = norm_gain[None, :]
    table = line_table(decay_rates, tokens)
    state = shape(heads, 128, 128)
    wide, narrow = shape(tokens, width), shape(tokens, width, dtype=BF16)
    tables = shape(heads, 2, BLOCK, BLOCK, dtype=BF16)
    state_near, wide_near = pltpu.VMEM(state.shape, F32), pltpu.VMEM(wide.shape, F32)
    far_q, far_k, far_v, far_grad = map(Streamed, (queries, key_rows, value_rows, out_grad))
    narrow_near, flags = pltpu.VMEM(narrow.shape, BF16), pltpu.SemaphoreType.DMA((2, 2))
    memory_end, memory_first = call(
        memory_kernel,
        "memory",
        (Far(state), state_near),
        Far(key_rows),
        Far(value_rows),
        grant=None,
        rates=decay_rates,
        scratch=(narrow_near, narrow_near, state_near, flags, pltpu.SemaphoreType.DMA((4,))),
    )
    probs, inside, aux = call(
        inside_kernel,
        "inside",
        (Streamed(tables), Streamed(wide), pltpu.VMEM((8, width), F32)),
        far_q,
        far_k,
        far_v,
        Streamed(gain),
        grant=None,
        rates=decay_rates,
    )
    entering = along_context(table, memory_end, False, aux)
    attention, sums = call(
        carried_kernel,
        "carried",
        (wide_near, pltpu.VMEM((lax.axis_size(SIDE), 8, 128), F32)),
        near(aux),
        near(queries),
        near(entering),
        near(memory_first),
        Far(inside),
        near(out_grad),
        grant=None,
        scratch=(wide_near, pltpu.SemaphoreType.DMA((2,))),
    )
    sums = lax.all_to_all(sums, SIDE, 0, 0)
    (backlog_end,) = call(
        functools.partial(grad_kernel, features),
        "grad",
        (Far(state),),
        near(aux),
        near(sums),
        near(queries),
        near(attention),
        near(out_grad),
        grant=None,
        scratch=(state_near, pltpu.SemaphoreType.DMA((4,))),
    )
    query_grad, normed_out, key_part, value_part, backlog_second = call(
        functools.partial(local_kernel, features),
        "local",
        (Streamed(narrow), Streamed(narrow), Streamed(wide), Streamed(wide), state_near),
        far_q,
        far_k,
        far_v,
        far_grad,
        Streamed(probs),
        near(entering),
        near(memory_first),
        near(sums),
        near(attention),
        Streamed(gain),
        grant=None,
        rates=decay_rates,
    )
    (settled,) = call(
        settle_kernel,
        "settle",
        (pltpu.VMEM((8, 128), F32),),
        near(key_part),
        near(value_part),
        near(backlog_second),
    )
    after = along_context(table, backlog_end, True, settled)
    key_grad, value_grad = call(
        finish_kernel,
        "finish",
        (Far(narrow), Far(narrow)),
        near(aux),
        near(key_rows),
        near(value_rows),
        near(key_part),
        near(value_part),
        near(after),
        near(backlog_second),
        scratch=(narrow_near, narrow_near, pltpu.SemaphoreType.DMA((8, 2))),
    )
    return (normed_out, query_grad, key_grad, value_grad)


def solution(mesh):
    split = Mesh(mesh.devices.reshape(4, 16, 4, 2), LINE + SIDE)
    rows = P(LINE, SIDE)
    return jax.shard_map(
        on_device,
        mesh=split,
        in_specs=(rows, rows, rows, P(SIDE), P(SIDE), rows),
        out_specs=(rows, rows, rows, rows),
        check_vma=False,
    )
```
